32 devices in a mesh: grp: 2 (over x), tok: 8 (over z, y), mdl: 2 (over core).
Axes of the slice: x: 2, y: 2, z: 4, core: 2. Of those that a mesh axis runs over, the one named last changes fastest.
Arguments:
- hidden: bfloat16 [1024, 4096], P(('grp', 'tok'), 'mdl'), parts along dimension 0, may hold values from -3 to 3
- queries: bfloat16 [1024, 16, 128], P(('grp', 'tok'), 'mdl'), parts along dimension 0, may hold values from -8 to 8
- cache: bfloat16 [16, 2048, 4, 2, 128], P(('grp', 'tok'), None, 'mdl'), parts along dimension 0, may hold values from -8 to 8
- cache_lengths: int32 [16], P(('grp', 'tok')), parts along dimension 0, may hold values from 128 to 2048, as said below
- wkv: bfloat16 [4096, 4, 2, 128], P('tok', 'mdl'), may hold values from -0.09375 to 0.09375
- wo: bfloat16 [16, 128, 4096], P('mdl', None, 'tok'), may hold values from -0.5 to 0.5
- attn_gain: bfloat16 [4096], replicated, may hold values from 0.5 to 1.5
- moe_gain: bfloat16 [4096], replicated, may hold values from 0.5 to 1.5
- w_gate: bfloat16 [16, 4096, 1792], P(('tok', 'mdl')), may hold values from -0.09375 to 0.09375
- w_up: bfloat16 [16, 4096, 1792], P(('tok', 'mdl')), may hold values from -0.09375 to 0.09375
- w_down: bfloat16 [16, 1792, 4096], P(('tok', 'mdl')), may hold values from -0.0625 to 0.0625
- expert_ids: int32 [1024, 2], P(('grp', 'tok', 'mdl')), parts along dimension 0, may hold values from 0 to 3, all different within a row; in each aligned block of 32 rows (0 to 31, 32 to 63, ...) at most 18 rows name the same one
- gates: float32 [1024, 2], P(('grp', 'tok', 'mdl')), parts along dimension 0, may hold values from 0.1 to 1
Outputs:
- mixed: bfloat16 [1024, 4096], P(('grp', 'tok', 'mdl')), parts along dimension 0
- fresh_key_value: bfloat16 [1024, 4, 2, 128], P(('grp', 'tok'), 'mdl'), parts along dimension 0
The draws below stay inside these ranges and needn't reach their ends.
There are 2 independent parts, one for each index of `grp`. The reference program is written for one: setup_inputs(seed, part) draws one part's arguments, and reference() takes and returns one part's arrays. A program takes and returns all parts, laid end to end along the dimension named above; an argument that names none is the same for every part. Nothing has to cross between parts.
Inputs may be any that keep to these rules, and one draw needn't show every extreme that they name: `expert_ids`: each token names 2 different experts; in aligned blocks of 32 rows no expert is named by more than 18 rows, a bound that some block reaches. `cache_lengths`: some rollout holds exactly 2048 cached positions.
All inputs are finite; a program needn't handle non-finite values.
Results may differ from the reference program's by a relative error of at most 0.007.
Values may be sent and summed in bfloat16 or wider, within the bound.
A program may use at most 128 MiB of HBM per device.

```python
import math
import jax
import jax.numpy as jnp
import numpy as np
from jax import lax

MODEL_DIM = 4096
HEAD_SIZE = 128
QUERY_HEADS = 16
KEY_VALUE_HEADS = 4
EXPERTS = 4
FF = 7168
TOPK = 2
NEW_TOKEN_SPAN = 64
CACHE_LIMIT = 2048
ROLLOUT_COUNT = 8
TOKEN_TOTAL = 512
TOK_MOE = 32
CAP = 18
SLABS = 4
FS = 1792
N_TOK = 8
N_MDL = 2


def draw_queries(key, part):
    array_shape = (TOKEN_TOTAL, QUERY_HEADS, HEAD_SIZE)
    return jnp.clip(jax.random.normal(jax.random.fold_in(key, 1), array_shape, jnp.float32) * 2.5, -7.5, 7.5).astype(jnp.bfloat16)


def draw_cache(key, part):
    array_shape = (ROLLOUT_COUNT, CACHE_LIMIT, KEY_VALUE_HEADS, 2, HEAD_SIZE)
    return jnp.clip(jax.random.normal(jax.random.fold_in(key, 2), array_shape, jnp.float32), -5.0, 5.0).astype(jnp.bfloat16)


def draw_cache_lengths(key, part):
    values = jax.random.randint(jax.random.fold_in(key, 3), (ROLLOUT_COUNT,), CACHE_LIMIT // 16, CACHE_LIMIT + 1)
    longest = jax.random.randint(jax.random.fold_in(key, 4), (), 0, ROLLOUT_COUNT)
    return jnp.where(jnp.arange(ROLLOUT_COUNT) == longest, CACHE_LIMIT, values).astype(jnp.int32)


def block_scale(stream_key, dims, split, smallest, top_value):
    level = 1.0
    for position, shards_of in split:
        steps = jax.random.uniform(jax.random.fold_in(jax.random.fold_in(stream_key, 6), position), (shards_of,), jnp.float32, smallest / len(split), top_value / len(split))
        level = level * jnp.repeat(jnp.exp(steps), dims[position] // shards_of).reshape((-1,) + (1,) * (len(dims) - 1 - position))
    return level


def routed_block(stream_key, own, number, rows, count, top, most, slope):
    ranking = jax.random.permutation(stream_key, count)
    crowded, usual = load_shares(count, rows * top, most, slope, True), load_shares(count, rows * top, most, slope, False)
    places = jnp.arange(count)

    def named(tallies, rotation):
        used = int((tallies > 0).sum())
        fixed = max(1, used // 4)
        shifted = fixed + (places - fixed + rotation * (used - fixed)) % max(1, count - fixed)
        return jnp.zeros((count,), jnp.int32).at[ranking[jnp.where(places < fixed, places, shifted)]].set(jnp.asarray(tallies, jnp.int32))

    tallies = jnp.where(number % 4 == 0, named(crowded, number // 4), named(usual, number - number // 4 - 1))
    mixed = jax.random.permutation(jax.random.fold_in(own, 3), count)
    source_of, receiver = mixed[0:count // 2 * 2:2], mixed[1:count // 2 * 2:2]
    room = jnp.minimum(tallies[source_of] - 1, most - tallies[receiver]) // 2
    room = jnp.where((source_of == ranking[0]) | (receiver == ranking[0]) | (tallies[receiver] == 0), 0, jnp.maximum(room, 0))
    shifted = jax.random.randint(jax.random.fold_in(own, 4), (count // 2,), 0, 1 << 20) % (room + 1)
    tallies = tallies.at[source_of].add(-shifted).at[receiver].add(shifted)
    items = jnp.searchsorted(jnp.cumsum(tallies), jnp.arange(rows * top), side="right").astype(jnp.int32)
    grid = items.reshape(top, rows).T
    grid = grid[jax.random.permutation(jax.random.fold_in(own, 1), rows)]
    rotation = jax.random.randint(jax.random.fold_in(own, 2), (rows, 1), 0, top)
    return jnp.take_along_axis(grid, (jnp.arange(top)[None, :] + rotation) % top, axis=1)


def load_shares(amount, total, reach, skew, full):
    weights = [(1 << 20) // math.isqrt(rank ** skew) + 1 for rank in range(1, amount + 1)]
    largest = reach if full else min(reach, max(-(-total // amount), total * weights[0] // sum(weights)))
    least = 1 if total - largest >= amount - 1 else 0
    holding, surplus = [largest] + [least] * (amount - 1), total - largest - least * (amount - 1)
    while surplus > 0:
        candidates = [i for i in range(1, amount) if holding[i] < largest] or [i for i in range(1, amount) if holding[i] < reach]
        whole, left = sum([weights[i] for i in candidates]), surplus
        for i in candidates:
            extra = min(reach - holding[i], max(1, left * weights[i] // whole), surplus)
            holding[i] = holding[i] + extra
            surplus = surplus - extra
    return np.array(holding)


def bell_draw(rng, shape, width, most, split=(), kind=jnp.bfloat16):
    drawn = width * jax.random.normal(rng, shape, jnp.float32)
    if split:
        drawn = drawn * block_scale(rng, shape, split, -0.22, 0.18)
    return jnp.clip(drawn, -most, most).astype(kind)


def setup_inputs(seed: int = 0, part: int = 0) -> dict:
    key_of = jax.random.split(jax.random.key(seed), 14)
    part_keys = jax.random.split(jax.random.fold_in(key_of[13], part), 14)
    hidden = bell_draw(part_keys[0], (TOKEN_TOTAL, MODEL_DIM), 0.5, 3.0, ((0, 8), (1, 2)))
    queries = draw_queries(jax.random.fold_in(jax.random.fold_in(key_of[13], part), 71), part)
    cache = draw_cache(jax.random.fold_in(jax.random.fold_in(key_of[13], part), 71), part)
    cache_lengths = draw_cache_lengths(jax.random.fold_in(jax.random.fold_in(key_of[13], part), 71), part)
    wkv = bell_draw(key_of[4], (MODEL_DIM, KEY_VALUE_HEADS, 2, HEAD_SIZE), MODEL_DIM ** -0.5, 0.09375, ((0, 8), (1, 2)))
    wo = bell_draw(key_of[5], (QUERY_HEADS, HEAD_SIZE, MODEL_DIM), HEAD_SIZE ** -0.5, 0.5, ((0, 2), (2, 8)))
    attn_gain = jnp.clip(1.0 + 0.1 * jax.random.normal(key_of[6], (MODEL_DIM,), jnp.float32), 0.5, 1.5).astype(jnp.bfloat16)
    moe_gain = jnp.clip(1.0 + 0.1 * jax.random.normal(key_of[7], (MODEL_DIM,), jnp.float32), 0.5, 1.5).astype(jnp.bfloat16)
    w_gate = bell_draw(key_of[8], (EXPERTS * SLABS, MODEL_DIM, FS), MODEL_DIM ** -0.5, 0.09375, ((0, 16),))
    w_up = bell_draw(key_of[9], (EXPERTS * SLABS, MODEL_DIM, FS), MODEL_DIM ** -0.5, 0.09375, ((0, 16),))
    w_down = bell_draw(key_of[10], (EXPERTS * SLABS, FS, MODEL_DIM), FF ** -0.5, 0.0625, ((0, 16),))
    expert_ids_keys = jax.random.split(jax.random.fold_in(part_keys[11], 1), TOKEN_TOTAL // TOK_MOE)
    expert_ids_turns = jax.random.permutation(jax.random.fold_in(part_keys[11], 3), TOKEN_TOTAL // TOK_MOE)
    expert_ids = jax.vmap(lambda own, number: routed_block(jax.random.fold_in(part_keys[11], 2), own, number, TOK_MOE, EXPERTS, TOPK, CAP, 2))(expert_ids_keys, expert_ids_turns).reshape((TOKEN_TOTAL, TOPK))
    gates = jnp.clip(0.1 + 0.9 * jax.random.uniform(part_keys[12], (TOKEN_TOTAL, TOPK), jnp.float32) ** block_scale(part_keys[12], (TOKEN_TOTAL, TOPK), ((0, 16),), -0.2, 0.2), 0.1, 1.0)
    return dict(hidden=hidden, queries=queries, cache=cache, cache_lengths=cache_lengths, wkv=wkv, wo=wo, attn_gain=attn_gain, moe_gain=moe_gain, w_gate=w_gate, w_up=w_up, w_down=w_down, expert_ids=expert_ids, gates=gates)


eps_norm = 1e-05
rope_base = 1000000.0
mask_fill = -1e+30

def rms_scale(values_in, gain):
    values = values_in.astype(jnp.float32)
    meansq = lax.optimization_barrier(jnp.mean(values * values, axis=-1, keepdims=True))
    return values * lax.rsqrt(meansq + eps_norm) * gain.astype(jnp.float32)

def rotate(key_rows, positions):
    half_dim = key_rows.shape[-1] // 2
    inverse = jnp.exp(jnp.arange(half_dim, dtype=jnp.float32) * (-2.0 * math.log(rope_base) / key_rows.shape[-1]))
    angle = positions.astype(jnp.float32)[:, None] * inverse[None, :]
    cosine = jnp.cos(angle)[:, None, :]
    sine_vals = jnp.sin(angle)[:, None, :]
    front_half = key_rows[..., :half_dim]
    back_half = key_rows[..., half_dim:]
    return jnp.concatenate([front_half * cosine - back_half * sine_vals, back_half * cosine + front_half * sine_vals], axis=-1)

def reference(hidden, queries, cache, cache_lengths, wkv, wo, attn_gain, moe_gain, w_gate, w_up, w_down, expert_ids, gates):
    normalized_input = rms_scale(hidden, attn_gain).astype(jnp.bfloat16)
    key_value_projection = jnp.dot(normalized_input, wkv.reshape(MODEL_DIM, KEY_VALUE_HEADS * 2 * HEAD_SIZE), preferred_element_type=jnp.float32).reshape(TOKEN_TOTAL, KEY_VALUE_HEADS, 2, HEAD_SIZE)
    positions = (cache_lengths[:, None] + jnp.arange(NEW_TOKEN_SPAN, dtype=jnp.int32)[None, :]).reshape(TOKEN_TOTAL).astype(jnp.int32)
    fresh_key_value = jnp.stack([rotate(key_value_projection[:, :, 0], positions), key_value_projection[:, :, 1]], axis=2).astype(jnp.bfloat16)
    head_group = QUERY_HEADS // KEY_VALUE_HEADS
    scale_factor = 1.0 / math.sqrt(HEAD_SIZE)
    query_all = queries.reshape(ROLLOUT_COUNT, NEW_TOKEN_SPAN, QUERY_HEADS, HEAD_SIZE)
    fresh_all_rows = fresh_key_value.reshape(ROLLOUT_COUNT, NEW_TOKEN_SPAN, KEY_VALUE_HEADS, 2, HEAD_SIZE)

    def one_rollout(packed):
        query_roll, cache_roll, new_roll, length = packed
        token_of_row = jnp.arange(NEW_TOKEN_SPAN * head_group) // head_group
        column = jnp.arange(CACHE_LIMIT + NEW_TOKEN_SPAN)
        allowed = jnp.where(column[None, :] < CACHE_LIMIT, column[None, :] < length, column[None, :] - CACHE_LIMIT <= token_of_row[:, None])
        outputs = []
        for head_index in range(KEY_VALUE_HEADS):
            query_rows = query_roll[:, head_index * head_group:(head_index + 1) * head_group].reshape(NEW_TOKEN_SPAN * head_group, HEAD_SIZE)
            key_rows = jnp.concatenate([cache_roll[:, head_index, 0], new_roll[:, head_index, 0]], axis=0)
            value_rows = jnp.concatenate([cache_roll[:, head_index, 1], new_roll[:, head_index, 1]], axis=0)
            scores = lax.dot_general(query_rows, key_rows, (((1,), (1,)), ((), ())), preferred_element_type=jnp.float32) * scale_factor
            scores = jnp.where(allowed, scores, mask_fill)
            row_max = lax.optimization_barrier(jnp.max(scores, axis=1, keepdims=True))
            weights = jnp.where(allowed, jnp.exp(scores - row_max), 0.0)
            probs = (weights / lax.optimization_barrier(jnp.sum(weights, axis=1, keepdims=True))).astype(jnp.bfloat16)
            attended = jnp.dot(probs, value_rows, preferred_element_type=jnp.float32).astype(jnp.bfloat16)
            outputs.append(attended.reshape(NEW_TOKEN_SPAN, head_group * HEAD_SIZE))
        return jnp.concatenate(outputs, axis=1)
    heads_out = lax.map(one_rollout, (query_all, cache, fresh_all_rows, cache_lengths)).reshape(TOKEN_TOTAL, QUERY_HEADS * HEAD_SIZE)
    attn_out = jnp.dot(heads_out, wo.reshape(QUERY_HEADS * HEAD_SIZE, MODEL_DIM), preferred_element_type=jnp.float32)
    resid = hidden.astype(jnp.float32) + attn_out
    moe_in = rms_scale(resid, moe_gain).astype(jnp.bfloat16)
    limit = N_TOK * N_MDL * CAP
    moe_out = jnp.zeros((TOKEN_TOTAL, MODEL_DIM), jnp.float32)
    for expert_idx in range(EXPERTS):
        match = expert_ids == expert_idx
        routed = jnp.any(match, axis=1)
        weight = lax.optimization_barrier(jnp.sum(jnp.where(match, gates, 0.0), axis=1)).astype(jnp.float32)
        order = jnp.argsort(jnp.where(routed, 0, 1).astype(jnp.int32), stable=True)[:limit].astype(jnp.int32)
        rows_in = moe_in[order]

        def slab_step(total, slab_idx):
            row_idx = expert_idx * SLABS + slab_idx
            gate_w = lax.dynamic_index_in_dim(w_gate, row_idx, 0, keepdims=False)
            up_w = lax.dynamic_index_in_dim(w_up, row_idx, 0, keepdims=False)
            down_w = lax.dynamic_index_in_dim(w_down, row_idx, 0, keepdims=False)
            gate_val = jnp.dot(rows_in, gate_w, preferred_element_type=jnp.float32)
            up_val = jnp.dot(rows_in, up_w, preferred_element_type=jnp.float32)
            slab_hidden = (jax.nn.silu(gate_val) * up_val).astype(jnp.bfloat16)
            slab_out = jnp.dot(slab_hidden, down_w, preferred_element_type=jnp.float32).astype(jnp.bfloat16)
            return (total + slab_out.astype(jnp.float32), None)
        total, unused = lax.scan(slab_step, jnp.zeros((limit, MODEL_DIM), jnp.float32), jnp.arange(SLABS, dtype=jnp.int32))
        moe_out = moe_out.at[order].add(weight[order][:, None] * total)
    mixed = (resid + moe_out).astype(jnp.bfloat16)
    return (mixed, fresh_key_value)
```

```python
import functools
import itertools
import math

import jax
import jax.numpy as jnp
from jax import lax
from jax.experimental import pallas as pl
from jax.experimental.pallas import tpu as pltpu
from jax.sharding import PartitionSpec as P

EXPERTS = 4
TOPK = 2


eps_norm = 1e-05
rope_base = 1000000.0
mask_fill = -1e30


def rms_scale(values_in, gain):
    values = values_in.astype(jnp.float32)
    meansq = jnp.mean(values * values, axis=-1, keepdims=True)
    return values * lax.rsqrt(meansq + eps_norm) * gain.astype(jnp.float32)


def rotate(key_rows, positions):
    half_dim = key_rows.shape[-1] // 2
    inverse = jnp.exp(
        jnp.arange(half_dim, dtype=jnp.float32) * (-2.0 * math.log(rope_base) / key_rows.shape[-1])
    )
    angle = positions.astype(jnp.float32)[:, None] * inverse[None, :]
    cosine = jnp.cos(angle)[:, None, :]
    sine_vals = jnp.sin(angle)[:, None, :]
    front_half = key_rows[..., :half_dim]
    back_half = key_rows[..., half_dim:]
    return jnp.concatenate(
        [front_half * cosine - back_half * sine_vals, back_half * cosine + front_half * sine_vals],
        axis=-1,
    )


def score_rows(query_rows, key_rows, scale_factor):
    return (
        lax.dot_general(
            query_rows, key_rows, (((1,), (1,)), ((), ())), preferred_element_type=jnp.float32
        )
        * scale_factor
    )


MESH = pl.DeviceIdType.MESH
LANES = 128
VMEM = pl.BlockSpec(memory_space=pltpu.VMEM)


def place(tok, mdl):
    return (lax.axis_index("grp"), tok, mdl)


def greet(peers):
    barrier = pltpu.get_barrier_semaphore()
    for peer in peers:
        pl.semaphore_signal(barrier, inc=1, device_id=peer, device_id_type=MESH)
    pl.semaphore_wait(barrier, len(peers))


def peers_of(groups, ranks, cores):
    tok, mdl = lax.axis_index("tok"), lax.axis_index("mdl")
    group, rank = tok // ranks, tok % ranks
    peers = [place((group + d) % groups * ranks + rank, mdl) for d in range(1, groups)]
    peers += [place(group * ranks + (rank + d) % ranks, mdl) for d in range(1, ranks)]
    if cores:
        peers.append(place(tok, 1 - mdl))
    return peers


def remote(src, dst, sems, index, device):
    copy = pltpu.make_async_remote_copy(
        src_ref=src,
        dst_ref=dst,
        send_sem=sems.at[0, index],
        recv_sem=sems.at[1, index],
        device_id=device,
        device_id_type=MESH,
    )
    copy.start()
    return copy


def near_first(count):
    return sorted(range(1, count), key=lambda d: (min(d, count - d), d))


def cut(width, pieces):
    part = width // pieces
    return [pl.ds(c * part, part) for c in range(pieces)]


def spread_kernel(groups, ranks, cores, same, pieces, send, out, sems, local_sem):
    tok, mdl = lax.axis_index("tok"), lax.axis_index("mdl")
    group, rank = tok // ranks, tok % ranks
    columns = cut(send.shape[-1], pieces)
    greet(peers_of(groups, ranks, cores))

    def piece(index, c):
        return send.at[:, columns[c]] if same else send.at[index, :, columns[c]]

    def slot(index, c):
        return out.at[index, mdl, :, columns[c]] if cores else out.at[index, :, columns[c]]

    started = []

    def go(src, dst, device):
        copy = remote(src, dst, sems, len(started), device)
        started.append(copy)
        return copy

    first, second, third = {}, [], []
    for c in range(pieces):
        for d in near_first(groups):
            there = (group + d) % groups
            first[c, d] = go(piece(there, c), slot(tok, c), place(there * ranks + rank, mdl))

    def onward(src, index, c):
        for d in near_first(ranks):
            there = group * ranks + (rank + d) % ranks
            second.append((d, index, c, go(src, slot(index, c), place(there, mdl))))

    def across(src, index, c):
        if cores:
            third.append(go(src, slot(index, c), place(tok, 1 - mdl)))

    for c in range(pieces):
        onward(piece(group, c), tok, c)
    for c in range(pieces):
        across(piece(group, c), tok, c)
    own = pltpu.make_async_copy(
        send if same else send.at[group], out.at[tok, mdl] if cores else out.at[tok], local_sem
    )
    own.start()
    for c in range(pieces):
        for d in near_first(groups):
            first[c, d].wait_recv()
            index = (group + groups - d) % groups * ranks + rank
            onward(slot(index, c), index, c)
            across(slot(index, c), index, c)
    for d, index, c, copy in second:
        copy.wait_recv()
        index = index // ranks * ranks + (rank + ranks - d) % ranks
        across(slot(index, c), index, c)
    for copy in third:
        copy.wait_recv()
    for copy in started:
        copy.wait_send()
    own.wait()


def spread(send, groups, ranks, cores, same, number, pieces=1):
    tiles = send.shape if same else send.shape[1:]
    toks = groups * ranks
    core_count = lax.axis_size("mdl") if cores else 1
    lead = (toks, core_count) if cores else (toks,)
    copies = pieces * (groups - 1 + groups * (ranks - 1) + (toks if cores else 0))
    return pl.pallas_call(
        functools.partial(spread_kernel, groups, ranks, cores, same, pieces),
        out_shape=jax.ShapeDtypeStruct(lead + tiles, send.dtype),
        in_specs=[VMEM],
        out_specs=VMEM,
        scratch_shapes=[pltpu.SemaphoreType.DMA((2, copies)), pltpu.SemaphoreType.DMA],
        compiler_params=pltpu.CompilerParams(
            collective_id=number, has_side_effects=True, vmem_limit_bytes=40 * 1024 * 1024
        ),
    )(send)


def collect_kernel(groups, ranks, pieces, parts, out, near, held, mid, sems):
    tok, mdl = lax.axis_index("tok"), lax.axis_index("mdl")
    group, rank = tok // ranks, tok % ranks
    columns = cut(parts.shape[-1], pieces)
    greet(peers_of(groups, ranks, True))
    started = []

    def go(src, dst, device):
        copy = remote(src, dst, sems, len(started), device)
        started.append(copy)
        return copy

    far = near_first(groups)[::-1] + [0]
    order = [(r, g) for r in near_first(ranks) + [0] for g in far]

    def index_of(r, g):
        return (group + g) % groups * ranks + (rank + r) % ranks

    across, second, last = {}, {}, []
    for c in range(pieces):
        for r, g in order:
            index = index_of(r, g)
            across[c, r, g] = go(
                parts.at[index, 1 - mdl, :, columns[c]],
                near.at[index, :, columns[c]],
                place(tok, 1 - mdl),
            )

    def both_cores(c, r, g):
        index = index_of(r, g)
        across[c, r, g].wait_recv()
        return parts[index, mdl, :, columns[c]].astype(jnp.float32) + near[
            index, :, columns[c]
        ].astype(jnp.float32)

    def to_ranks(c):
        for r, g in order:
            if r == 0:
                continue
            index = index_of(r, g)
            held[index, :, columns[c]] = both_cores(c, r, g).astype(held.dtype)
            second[c, r, g] = go(
                held.at[index, :, columns[c]],
                mid.at[r - 1, g, :, columns[c]],
                place(group * ranks + (rank + r) % ranks, mdl),
            )

    def to_sources(c):
        for g in far:
            index = index_of(0, g)
            total = both_cores(c, 0, g)
            for r in range(1, ranks):
                second[c, r, g].wait_recv()
                total = total + mid[r - 1, g, :, columns[c]].astype(jnp.float32)
            if g == 0:
                out[group, :, columns[c]] = total.astype(out.dtype)
            else:
                held[index, :, columns[c]] = total.astype(held.dtype)
                last.append(
                    go(
                        held.at[index, :, columns[c]],
                        out.at[group, :, columns[c]],
                        place((group + g) % groups * ranks + rank, mdl),
                    )
                )

    for c in range(pieces + 1):
        if c < pieces:
            to_ranks(c)
        if c > 0:
            to_sources(c - 1)
    for copy in last:
        copy.wait_recv()
    for copy in started:
        copy.wait_send()


def collect(parts, groups, ranks, number, pieces=1):
    toks = groups * ranks
    tile = parts.shape[2:]
    copies = pieces * (toks + groups * (ranks - 1) + groups - 1)
    return pl.pallas_call(
        functools.partial(collect_kernel, groups, ranks, pieces),
        out_shape=jax.ShapeDtypeStruct((groups,) + tile, parts.dtype),
        in_specs=[VMEM],
        out_specs=VMEM,
        scratch_shapes=[
            pltpu.VMEM((toks,) + tile, parts.dtype),
            pltpu.VMEM((toks,) + tile, parts.dtype),
            pltpu.VMEM((max(ranks - 1, 1), groups) + tile, parts.dtype),
            pltpu.SemaphoreType.DMA((2, copies)),
        ],
        compiler_params=pltpu.CompilerParams(
            collective_id=number, has_side_effects=True, vmem_limit_bytes=40 * 1024 * 1024
        ),
    )(parts)


def divide(width, choices=(256, 128)):
    for part in choices:
        if width % part == 0 and width // part >= 1:
            return part
    return width


def moe_kernel(
    groups,
    ranks,
    cores,
    pieces,
    depths,
    tokens,
    select,
    resid,
    weights,
    gate_hbm,
    up_hbm,
    down_hbm,
    mixed,
    send,
    recv,
    near,
    mid,
    home,
    rows,
    gate_w,
    up_w,
    down_w,
    found,
    gate_acc,
    up_acc,
    slab,
    sems,
    load_sems,
    own_sem,
):
    tok, mdl = lax.axis_index("tok"), lax.axis_index("mdl")
    group, rank = tok // ranks, tok % ranks
    toks = groups * ranks
    main = send.shape[1]
    cap = select.shape[0] // groups
    rest = cap - main
    width = tokens.shape[1]
    hidden = slab.shape[1]
    part = width // pieces
    columns = cut(width, pieces)
    packed = cut(send.shape[2], pieces)
    blocks = rest * part // main // LANES * (main // rest)
    main_rows = cores * toks * main

    def pack(target, lead, rows_in, row, c):
        for b in range(blocks):
            spot, lane = divmod(b, main // rest)
            at = c * (send.shape[2] // pieces) + part + spot * LANES
            target[(*lead, pl.ds(lane * rest, rest), pl.ds(at, LANES))] = rows_in[
                row : row + rest, b * LANES : (b + 1) * LANES
            ]

    def unpack(target, row, source, lead, c):
        for b in range(blocks):
            spot, lane = divmod(b, main // rest)
            at = c * (send.shape[2] // pieces) + part + spot * LANES
            target[row : row + rest, b * LANES : (b + 1) * LANES] = source[
                (*lead, pl.ds(lane * rest, rest), pl.ds(at, LANES))
            ]

    def body(c):
        return pl.ds(c * (send.shape[2] // pieces), part)

    tile = divide(hidden)

    loads = {}

    def load(name, c, src, dst):
        copy = pltpu.make_async_copy(src, dst, load_sems.at[len(loads)])
        copy.start()
        loads[name, c] = copy

    for c in range(pieces):
        load("gate", c, gate_hbm.at[0, columns[c], :], gate_w.at[columns[c], :])
        load("up", c, up_hbm.at[0, columns[c], :], up_w.at[columns[c], :])
    for c in range(pieces):
        load("down", c, down_hbm.at[0, :, columns[c]], down_w.at[c])

    greet(peers_of(groups, ranks, True))
    started = []
    numbers = itertools.count()

    def go(src, dst, device):
        copy = remote(src, dst, sems, next(numbers), device)
        started.append(copy)
        return copy

    other = place(tok, 1 - mdl)

    def rank_place(r):
        return place(group * ranks + (rank + r) % ranks, mdl)

    def group_place(g):
        return place((group + g) % groups * ranks + rank, mdl)

    far = near_first(groups)
    near_ranks = near_first(ranks)
    by_group, by_rank, by_core = {}, {}, {}
    for c in range(pieces):
        picked = jnp.dot(
            select[...], tokens[:, columns[c]], preferred_element_type=jnp.float32
        ).astype(send.dtype)
        for e in range(groups):
            send[e, :, body(c)] = picked[e * main : (e + 1) * main]
            pack(send, (e,), picked, groups * main + e * rest, c)
        for d in far:
            by_group[c, d] = go(
                send.at[(group + d) % groups, :, packed[c]],
                recv.at[mdl, group, rank, :, packed[c]],
                group_place(d),
            )
        for r in near_ranks:
            by_rank[c, 0, r] = go(
                send.at[group, :, packed[c]],
                recv.at[mdl, group, rank, :, packed[c]],
                rank_place(r),
            )
        by_core[c, 0, 0] = go(
            send.at[group, :, packed[c]], recv.at[mdl, group, rank, :, packed[c]], other
        )

    own = pltpu.make_async_copy(send.at[group], recv.at[mdl, group, rank], own_sem)
    own.start()

    def from_groups(c):
        for d in far:
            by_group[c, d].wait_recv()
            source = (group + groups - d) % groups
            block = recv.at[mdl, source, rank, :, packed[c]]
            for r in near_ranks:
                by_rank[c, d, r] = go(block, block, rank_place(r))
            by_core[c, d, 0] = go(block, block, other)

    def from_ranks(c):
        for d in [0] + far:
            for r in near_ranks:
                by_rank[c, d, r].wait_recv()
                source = (group + groups - d) % groups
                giver = (rank + ranks - r) % ranks
                block = recv.at[mdl, source, giver, :, packed[c]]
                by_core[c, d, r] = go(block, block, other)

    def assemble(c):
        for d in [0] + far:
            for r in [0] + near_ranks:
                by_core[c, d, r].wait_recv()
        if c == 0:
            own.wait()
        rows[0:main_rows, :] = recv[:, :, :, :, body(c)].reshape(main_rows, part)
        spot = main_rows
        for m in range(cores):
            for g in range(groups):
                for r in range(ranks):
                    unpack(rows, spot, recv, (m, g, r), c)
                    spot += rest

    def project(c):
        assemble(c)
        loads["gate", c].wait()
        loads["up", c].wait()

        def step(n, carry):
            at = pl.ds(pl.multiple_of(n * tile, tile), tile)
            x = rows[...]
            gate_val = jnp.dot(x, gate_w[columns[c], at], preferred_element_type=jnp.float32)
            up_val = jnp.dot(x, up_w[columns[c], at], preferred_element_type=jnp.float32)
            if c > 0:
                gate_val = gate_val + gate_acc[:, at]
                up_val = up_val + up_acc[:, at]
            if c < pieces - 1:
                gate_acc[:, at] = gate_val
                up_acc[:, at] = up_val
            else:
                slab[:, at] = (gate_val / (1.0 + jnp.exp(-gate_val)) * up_val).astype(slab.dtype)
            return carry

        lax.fori_loop(0, hidden // tile, step, 0)

    for s in range(pieces + 2):
        if s < pieces:
            from_groups(s)
        if 0 <= s - 1 < pieces:
            from_ranks(s - 1)
        if 0 <= s - 2 < pieces:
            project(s - 2)

    for copy in started:
        copy.wait_send()
    started.clear()
    down_tile = divide(part)
    across, to_rank, to_home = {}, {}, {}

    def down(c):
        loads["down", c].wait()

        def step(n, carry):
            at = pl.multiple_of(n * down_tile, down_tile)
            rows[:, pl.ds(at, down_tile)] = jnp.dot(
                slab[...],
                down_w[c, :, pl.ds(at, down_tile)],
                preferred_element_type=jnp.float32,
            ).astype(rows.dtype)
            return carry

        lax.fori_loop(0, part // down_tile, step, 0)
        recv[:, :, :, :, body(c)] = rows[0:main_rows, :].reshape(cores, groups, ranks, main, part)
        spot = main_rows
        for m in range(cores):
            for g in range(groups):
                for r in range(ranks):
                    pack(recv, (m, g, r), rows, spot, c)
                    spot += rest
        across[c] = go(
            recv.at[1 - mdl, :, :, :, packed[c]], near.at[:, :, :, packed[c]], other
        )

    def pair(g, r, c):
        return recv[mdl, g, r, :, packed[c]].astype(jnp.float32) + near[
            g, r, :, packed[c]
        ].astype(jnp.float32)

    def to_ranks(c):
        across[c].wait_recv()
        for r in near_ranks:
            there = (rank + r) % ranks
            for g in range(groups):
                recv[mdl, g, there, :, packed[c]] = pair(g, there, c).astype(recv.dtype)
            to_rank[c, r] = go(
                recv.at[mdl, :, there, :, packed[c]], mid.at[r - 1, :, :, packed[c]], rank_place(r)
            )

    def to_sources(c):
        for r in near_ranks:
            to_rank[c, r].wait_recv()
        for d in far[::-1] + [0]:
            there = (group + d) % groups
            total = pair(there, rank, c)
            for r in near_ranks:
                total = total + mid[r - 1, there, :, packed[c]].astype(jnp.float32)
            if d == 0:
                home[group, :, packed[c]] = total.astype(home.dtype)
            else:
                recv[mdl, there, rank, :, packed[c]] = total.astype(recv.dtype)
                to_home[c, d] = go(
                    recv.at[mdl, there, rank, :, packed[c]],
                    home.at[group, :, packed[c]],
                    group_place(d),
                )

    def finish(c):
        for d in far:
            to_home[c, d].wait_recv()
        found[0 : groups * main, :] = home[:, :, body(c)].reshape(groups * main, part)
        for e in range(groups):
            unpack(found, groups * main + e * rest, home, (e,), c)
        terms = jnp.dot(weights[...], found[...], preferred_element_type=jnp.float32)
        total = resid[:, columns[c]]
        for k in range(weights.shape[0] // resid.shape[0]):
            total = total + terms[k * resid.shape[0] : (k + 1) * resid.shape[0]]
        mixed[:, columns[c]] = total.astype(mixed.dtype)

    lag_rank, lag_source, lag_end = depths
    for s in range(pieces + lag_end):
        if s < pieces:
            down(s)
        if 0 <= s - lag_rank < pieces:
            to_ranks(s - lag_rank)
        if 0 <= s - lag_source < pieces:
            to_sources(s - lag_source)
        if 0 <= s - lag_end < pieces:
            finish(s - lag_end)
    for copy in started:
        copy.wait_send()


def experts(
    tokens, select, resid, weights, w_gate, w_up, w_down, groups, ranks, cores, number, pieces=4
):
    width = tokens.shape[1]
    toks = groups * ranks
    cap = select.shape[0] // groups
    main = cap // 16 * 16
    packed = width // main * cap
    depth, hidden = w_gate.shape[1:]
    part = width // pieces
    dtype = tokens.dtype
    copies = pieces * ((groups - 1) * 2 + (groups + 1) * (ranks - 1) + toks + 1)
    total_rows = cores * toks * cap
    return pl.pallas_call(
        functools.partial(moe_kernel, groups, ranks, cores, pieces, (1, 2, 4)),
        out_shape=jax.ShapeDtypeStruct(resid.shape, dtype),
        in_specs=[VMEM] * 4 + [pl.BlockSpec(memory_space=pl.ANY)] * 3,
        out_specs=VMEM,
        scratch_shapes=[
            pltpu.VMEM((groups, main, packed), dtype),
            pltpu.VMEM((cores, groups, ranks, main, packed), dtype),
            pltpu.VMEM((groups, ranks, main, packed), dtype),
            pltpu.VMEM((max(ranks - 1, 1), groups, main, packed), dtype),
            pltpu.VMEM((groups, main, packed), dtype),
            pltpu.VMEM((total_rows, part), dtype),
            pltpu.VMEM((depth, hidden), dtype),
            pltpu.VMEM((depth, hidden), dtype),
            pltpu.VMEM((pieces, hidden, part), dtype),
            pltpu.VMEM((groups * cap, part), dtype),
            pltpu.VMEM((total_rows, hidden), jnp.float32),
            pltpu.VMEM((total_rows, hidden), jnp.float32),
            pltpu.VMEM((total_rows, hidden), dtype),
            pltpu.SemaphoreType.DMA((2, copies)),
            pltpu.SemaphoreType.DMA((3 * pieces,)),
            pltpu.SemaphoreType.DMA,
        ],
        compiler_params=pltpu.CompilerParams(
            collective_id=number, has_side_effects=True, vmem_limit_bytes=67043328
        ),
    )(tokens, select, resid, weights, w_gate, w_up, w_down)


def attention_kernel(length, queries, cached, fresh, out):
    heads, span, width = queries.shape
    rows = heads * span
    query_rows = queries[...].reshape(rows, width)
    scale_factor = 1.0 / math.sqrt(width)
    limit = cached.shape[2]
    block = min(512, limit)
    token = lax.broadcasted_iota(jnp.int32, (rows, span), 0) % span
    column = lax.broadcasted_iota(jnp.int32, (rows, span), 1)
    scores = [
        jnp.where(
            column <= token, score_rows(query_rows, fresh[0, 0], scale_factor), mask_fill
        )
    ]
    values = [fresh[0, 1]]
    for start in range(0, limit, block):
        position = lax.broadcasted_iota(jnp.int32, (rows, block), 1) + start
        found = score_rows(query_rows, cached[0, 0, pl.ds(start, block)], scale_factor)
        scores.append(jnp.where(position < length[0], found, mask_fill))
        values.append(cached[0, 1, pl.ds(start, block)])
    top = functools.reduce(jnp.maximum, [jnp.max(x, axis=1, keepdims=True) for x in scores])
    total = jnp.zeros((rows, 1), jnp.float32)
    mixed = jnp.zeros((rows, width), jnp.float32)
    for found, value_rows in zip(scores, values):
        weights = jnp.exp(found - top)
        total += jnp.sum(weights, axis=1, keepdims=True)
        mixed += jnp.dot(
            weights.astype(jnp.bfloat16), value_rows, preferred_element_type=jnp.float32
        )
    attended = (mixed / total).astype(out.dtype)
    for head in range(heads):
        out[:, head * width : (head + 1) * width] = attended[head * span : (head + 1) * span]


def attention(queries, cache, lengths, fresh):
    span, query_heads, width = queries.shape
    kv_heads = cache.shape[2]
    per_head = query_heads // kv_heads
    limit = cache.shape[1]
    return pl.pallas_call(
        attention_kernel,
        grid=(kv_heads,),
        out_shape=jax.ShapeDtypeStruct((span, query_heads * width), jnp.bfloat16),
        in_specs=[
            pl.BlockSpec(memory_space=pltpu.SMEM),
            pl.BlockSpec((per_head, span, width), lambda h: (h, 0, 0)),
            pl.BlockSpec((1, 2, limit, width), lambda h: (h, 0, 0, 0)),
            pl.BlockSpec((1, 2, span, width), lambda h: (h, 0, 0, 0)),
        ],
        out_specs=pl.BlockSpec((span, per_head * width), lambda h: (0, h)),
        compiler_params=pltpu.CompilerParams(vmem_limit_bytes=40 * 1024 * 1024),
    )(
        lengths,
        queries.transpose(1, 0, 2),
        cache[0].transpose(1, 2, 0, 3),
        fresh.transpose(1, 2, 0, 3),
    )


def shards(
    hidden,
    queries,
    cache,
    cache_lengths,
    wkv,
    wo,
    attn_gain,
    moe_gain,
    w_gate,
    w_up,
    w_down,
    expert_ids,
    gates,
):
    full_rows = lax.all_gather(hidden, "mdl", axis=1, tiled=True)
    span_len = full_rows.shape[0]
    toks = lax.axis_size("tok")
    core_count = lax.axis_size("mdl")
    ranks = toks // EXPERTS
    core_rows = span_len // core_count
    core_start = lax.axis_index("mdl") * core_rows
    own_rows = lax.dynamic_slice_in_dim(full_rows, core_start, core_rows, 0)
    normalized_input = rms_scale(own_rows, attn_gain).astype(jnp.bfloat16)
    kv_heads = wkv.shape[1]
    head_dim = wkv.shape[3]
    depth = wkv.shape[0]
    slices = normalized_input.reshape(core_rows, toks, depth).transpose(1, 0, 2)
    every_row = spread(slices, toks, 1, True, False, 1).reshape(-1, depth)
    partial_kv = jnp.dot(
        every_row, wkv.reshape(depth, -1), preferred_element_type=jnp.float32
    ).astype(jnp.bfloat16)
    terms = spread(partial_kv.reshape(toks, span_len, -1), toks, 1, False, False, 2)
    key_value_projection = jnp.sum(terms.astype(jnp.float32), axis=0).reshape(
        span_len, kv_heads, 2, head_dim
    )
    length = cache_lengths[0]
    positions = length + jnp.arange(span_len, dtype=jnp.int32)
    fresh_key_value = jnp.stack(
        [rotate(key_value_projection[:, :, 0], positions), key_value_projection[:, :, 1]], axis=2
    ).astype(jnp.bfloat16)
    heads_out = attention(queries, cache, cache_lengths, fresh_key_value)
    every_head = spread(heads_out, EXPERTS, ranks, False, True, 3, 2)
    attn_part = jnp.dot(
        every_head.reshape(toks * span_len, -1),
        wo.reshape(-1, wo.shape[2]),
        preferred_element_type=jnp.float32,
    ).astype(jnp.bfloat16)
    attn_rows = collect(
        attn_part.reshape(toks, core_count, core_rows, -1), toks, 1, 4
    )
    attn_rows = attn_rows.transpose(1, 0, 2).reshape(core_rows, -1).astype(jnp.float32)
    resid = own_rows.astype(jnp.float32) + attn_rows
    moe_in = rms_scale(resid, moe_gain).astype(jnp.bfloat16)
    expert_range = jnp.arange(EXPERTS)
    matches = expert_ids[:, :, None] == expert_range[None, None, :]
    chosen = jnp.sum(matches.astype(jnp.int32), axis=1)
    route = jnp.sum(jnp.where(matches, gates[:, :, None], 0.0), axis=1)
    slot_of = jnp.cumsum(chosen, axis=0) - chosen
    capacity = core_rows * TOPK * 9 // (8 * EXPERTS)
    slot_range = jnp.arange(capacity)
    select = (slot_of.T[:, None, :] == slot_range[None, :, None]) & (chosen.T[:, None, :] > 0)
    main = capacity // 16 * 16

    def by_tile(table):
        return jnp.concatenate(
            [
                table[:, :main].reshape(EXPERTS * main, core_rows),
                table[:, main:].reshape(EXPERTS * (capacity - main), core_rows),
            ]
        )

    picks = by_tile(select.astype(jnp.float32))
    table = by_tile(select.astype(jnp.float32) * route.T[:, None, :]).T
    first = table.astype(jnp.bfloat16)
    second = (table - first.astype(jnp.float32)).astype(jnp.bfloat16)
    third = (table - first.astype(jnp.float32) - second.astype(jnp.float32)).astype(jnp.bfloat16)
    weights = jnp.concatenate([first, second, third])
    mixed = experts(
        moe_in,
        picks.astype(jnp.bfloat16),
        resid,
        weights,
        w_gate,
        w_up,
        w_down,
        EXPERTS,
        ranks,
        core_count,
        5,
    )
    return (mixed, fresh_key_value)


def solution(mesh):
    in_specs = (
        P(("grp", "tok"), "mdl"),
        P(("grp", "tok"), "mdl", None),
        P(("grp", "tok"), None, "mdl", None, None),
        P(("grp", "tok")),
        P("tok", "mdl", None, None),
        P("mdl", None, "tok"),
        P(),
        P(),
        P(("tok", "mdl"), None, None),
        P(("tok", "mdl"), None, None),
        P(("tok", "mdl"), None, None),
        P(("grp", "tok", "mdl"), None),
        P(("grp", "tok", "mdl"), None),
    )
    out_specs = (P(("grp", "tok", "mdl"), None), P(("grp", "tok"), "mdl", None, None))
    return jax.shard_map(shards, mesh=mesh, in_specs=in_specs, out_specs=out_specs, check_vma=False)
```

```python
import functools
import itertools
import math

import jax
import jax.numpy as jnp
from jax import lax
from jax.experimental import pallas as pl
from jax.experimental.pallas import tpu as pltpu
from jax.sharding import PartitionSpec as P

EXPERTS = 4
TOPK = 2
PIECES = 4


eps_norm = 1e-05
rope_base = 1000000.0
mask_fill = -1e30


def rotation(head_dim, positions):
    half_dim = head_dim // 2
    inverse = jnp.exp(
        jnp.arange(half_dim, dtype=jnp.float32) * (-2.0 * math.log(rope_base) / head_dim)
    )
    angle = positions.astype(jnp.float32)[:, None] * inverse[None, :]
    cosine, sine = jnp.cos(angle), jnp.sin(angle)
    return jnp.concatenate([cosine, cosine], axis=1), jnp.concatenate([-sine, sine], axis=1)


def score_rows(query_rows, key_rows, scale_factor):
    return (
        lax.dot_general(
            query_rows, key_rows, (((1,), (1,)), ((), ())), preferred_element_type=jnp.float32
        )
        * scale_factor
    )


MESH = pl.DeviceIdType.MESH
LANES = 128
VMEM = pl.BlockSpec(memory_space=pltpu.VMEM)


def place(tok, mdl):
    return (lax.axis_index("grp"), tok, mdl)


def greet(peers):
    barrier = pltpu.get_barrier_semaphore()
    for peer in peers:
        pl.semaphore_signal(barrier, inc=1, device_id=peer, device_id_type=MESH)
    pl.semaphore_wait(barrier, len(peers))


def peers_of(groups, ranks, cores):
    tok, mdl = lax.axis_index("tok"), lax.axis_index("mdl")
    group, rank = tok // ranks, tok % ranks
    peers = [place((group + d) % groups * ranks + rank, mdl) for d in range(1, groups)]
    peers += [place(group * ranks + (rank + d) % ranks, mdl) for d in range(1, ranks)]
    if cores:
        peers.append(place(tok, 1 - mdl))
    return peers


def remote(src, dst, sems, index, device):
    copy = pltpu.make_async_remote_copy(
        src_ref=src,
        dst_ref=dst,
        send_sem=sems.at[0, index],
        recv_sem=sems.at[1, index],
        device_id=device,
        device_id_type=MESH,
    )
    copy.start()
    return copy


def near_first(count):
    return sorted(range(1, count), key=lambda d: (min(d, count - d), d))


def cut(width, pieces):
    part = width // pieces
    return [pl.ds(c * part, part) for c in range(pieces)]


def divide(width, choices=(256, 128)):
    for part in choices:
        if width % part == 0 and width // part >= 1:
            return part
    return width


def layer_kernel(
    dims,
    lengths,
    hidden,
    queries,
    cosines,
    sines,
    attn_gain,
    moe_gain,
    select,
    weights,
    cache_hbm,
    wkv_hbm,
    wo_hbm,
    gate_hbm,
    up_hbm,
    down_hbm,
    mixed,
    fresh,
    full,
    slices,
    own_square,
    other_square,
    part_kv,
    mid_kv,
    sum_kv,
    in_kv,
    cache,
    wkv,
    wo,
    tops,
    sums,
    heads_acc,
    heads,
    part_out,
    near_out,
    in_out,
    resid,
    send,
    recv,
    near,
    mid,
    home,
    rows,
    gate_w,
    up_w,
    down_w,
    gate_acc,
    up_acc,
    slab,
    sems,
    load_sems,
):
    groups, ranks, cores, pieces = dims
    tok, mdl = lax.axis_index("tok"), lax.axis_index("mdl")
    group, rank = tok // ranks, tok % ranks
    toks = groups * ranks
    f32, narrow = jnp.float32, jnp.bfloat16

    width = full.shape[1]
    part = width // pieces
    columns = cut(width, pieces)
    loads = {}

    def load(src, dst, *name):
        copy = pltpu.make_async_copy(src, dst, load_sems.at[len(loads)])
        copy.start()
        loads[name] = copy

    load(wkv_hbm, wkv, "wkv")
    for h in range(cache.shape[0]):
        load(cache_hbm.at[h], cache.at[h], "cache", h)
    load(wo_hbm, wo, "wo")

    numbers = itertools.count()
    started = []
    other = place(tok, 1 - mdl)
    far = near_first(groups)
    near_ranks = near_first(ranks)
    every_rank = [0] + near_ranks

    def go(src, dst, device):
        copy = remote(src, dst, sems, next(numbers), device)
        started.append(copy)
        return copy

    def all_sent():
        for copy in started:
            copy.wait_send()
        started.clear()

    def rank_place(r):
        return place(group * ranks + (rank + r) % ranks, mdl)

    def group_place(g):
        return place((group + g) % groups * ranks + rank, mdl)

    def group_from(d):
        return (group + groups - d) % groups

    def rank_from(r):
        return (rank + ranks - r) % ranks

    greet(peers_of(toks, 1, True))

    span, features = hidden.shape
    half = span // cores
    depth = width // toks

    def lines(core):
        return pl.ds(pl.multiple_of(core * half, half), half)

    def half_features(core):
        return pl.ds(pl.multiple_of(core * features, features), features)

    swap = go(hidden.at[lines(1 - mdl), :], full.at[:, half_features(mdl)], other)
    full[:, half_features(mdl)] = hidden[lines(mdl), :]
    values = hidden[...].astype(f32)
    square = jnp.sum(values * values, axis=1, keepdims=True)
    own_square[...] = jnp.broadcast_to(square, own_square.shape)
    swap_square = go(own_square, other_square, other)
    for c in range(pieces):
        load(gate_hbm.at[0, columns[c], :], gate_w.at[columns[c], :], "gate", c)
        load(up_hbm.at[0, columns[c], :], up_w.at[columns[c], :], "up", c)
    for c in range(pieces):
        load(down_hbm.at[0, :, columns[c]], down_w.at[c], "down", c)
    swap.wait_recv()

    def slice_of(target):
        return pl.ds(pl.multiple_of(target * depth, depth), depth)

    outward, twin = {}, {}
    for d in [0] + far:
        for r in every_rank:
            target = (group + d) % groups * ranks + (rank + r) % ranks
            if d or r:
                outward[d, r] = go(
                    full.at[:, slice_of(target)],
                    slices.at[group, rank, mdl],
                    place(target, mdl),
                )
    slices[group, rank, mdl] = full[:, slice_of(tok)]
    twin[0, 0] = go(full.at[:, slice_of(tok)], slices.at[group, rank, mdl], other)

    query_heads, _, head_dim = queries.shape
    kv_heads = cache.shape[0]
    per_head = query_heads // kv_heads
    scale_factor = 1.0 / math.sqrt(head_dim)
    limit = cache.shape[2]
    block = min(512, limit)
    query_count = per_head * span

    def query_rows(h):
        return queries[h * per_head : (h + 1) * per_head].reshape(query_count, head_dim)

    def cached_attention(h):
        loads["cache", h].wait()
        asked = query_rows(h)
        scores, values = [], []
        for start in range(0, limit, block):
            position = lax.broadcasted_iota(jnp.int32, (query_count, block), 1) + start
            score = score_rows(asked, cache[h, 0, pl.ds(start, block)], scale_factor)
            scores.append(jnp.where(position < lengths[0], score, mask_fill))
            values.append(cache[h, 1, pl.ds(start, block)])
        top = functools.reduce(jnp.maximum, [jnp.max(x, axis=1, keepdims=True) for x in scores])
        total = jnp.zeros((query_count, 1), f32)
        found_values = jnp.zeros((query_count, head_dim), f32)
        for score, value_rows in zip(scores, values):
            chance = jnp.exp(score - top)
            total += jnp.sum(chance, axis=1, keepdims=True)
            found_values += jnp.dot(chance.astype(narrow), value_rows, preferred_element_type=f32)
        tops[h] = jnp.broadcast_to(top, (query_count, head_dim))
        sums[h] = jnp.broadcast_to(total, (query_count, head_dim))
        heads_acc[h] = found_values

    cached_attention(0)

    kv_width = wkv.shape[1]
    gain_slice = attn_gain[:, slice_of(tok)].astype(f32)
    loads["wkv",].wait()
    kv_rank, kv_home = {}, {}

    def project_kv(d):
        source = group_from(d)
        for r in every_rank:
            if d or r:
                outward[d, r].wait_recv()
                landed = slices.at[source, rank_from(r), mdl]
                twin[d, r] = go(landed, landed, other)
        for r in every_rank:
            twin[d, r].wait_recv()
        taken = slices[source].reshape(ranks * span, depth).astype(f32) * gain_slice
        part_kv[source] = (
            jnp.dot(taken.astype(narrow), wkv[...], preferred_element_type=f32)
            .astype(narrow)
            .reshape(ranks, span, kv_width)
        )
        for r in near_ranks:
            kv_rank[d, r] = go(
                part_kv.at[source, (rank + r) % ranks], mid_kv.at[r - 1, source], rank_place(r)
            )

    def reduce_kv(d):
        source = group_from(d)
        total = part_kv[source, rank].astype(f32)
        for r in near_ranks:
            kv_rank[d, r].wait_recv()
            total = total + mid_kv[r - 1, source].astype(f32)
        if d:
            sum_kv[source] = total.astype(narrow)
            kv_home[d] = go(sum_kv.at[source], in_kv.at[group], group_place(-d))
        else:
            in_kv[group] = total.astype(narrow)

    order = [0] + far
    for s in range(groups + 1):
        if s < groups:
            project_kv(order[s])
        if s > 0:
            reduce_kv(order[s - 1])
    for h in range(1, kv_heads):
        cached_attention(h)
    swap_square.wait_recv()
    meansq = (own_square[...] + other_square[...]) * (1.0 / width)
    row_scale = lax.rsqrt(meansq + eps_norm)
    for d in far:
        kv_home[d].wait_recv()

    token = lax.broadcasted_iota(jnp.int32, (query_count, span), 0) % span
    column = lax.broadcasted_iota(jnp.int32, (query_count, span), 1)
    head_width = per_head * head_dim
    head_columns = [pl.ds(h * head_width, head_width) for h in range(kv_heads)]
    head_group, head_rank = {}, {}
    for h in range(kv_heads):
        pair_of = []
        for kind in range(2):
            at = pl.ds((2 * h + kind) * head_dim, head_dim)
            total = in_kv[0, :, at].astype(f32)
            for g in range(1, groups):
                total = total + in_kv[g, :, at].astype(f32)
            total = total * row_scale
            if kind == 0:
                total = total * cosines[...] + pltpu.roll(total, head_dim // 2, 1) * sines[...]
            pair_of.append(total.astype(narrow))
            fresh[:, at] = pair_of[kind]
        score = score_rows(query_rows(h), pair_of[0], scale_factor)
        score = jnp.where(column <= token, score, mask_fill)
        before = tops[h]
        top = jnp.maximum(before, jnp.max(score, axis=1, keepdims=True))
        fade = jnp.exp(before - top)
        chance = jnp.exp(score - top[:, :1])
        total = sums[h] * fade + jnp.sum(chance, axis=1, keepdims=True)
        attended = heads_acc[h] * fade + jnp.dot(
            chance.astype(narrow), pair_of[1], preferred_element_type=f32
        )
        attended = (attended / total).astype(narrow)
        for head in range(per_head):
            at = pl.ds(h * head_width + head * head_dim, head_dim)
            heads[group, rank, :, at] = attended[head * span : (head + 1) * span]
        own = heads.at[group, rank, :, head_columns[h]]
        for d in far:
            head_group[h, d] = go(own, own, group_place(d))
        for r in near_ranks:
            head_rank[h, 0, r] = go(own, own, rank_place(r))

    out_width = wo.shape[1]
    loads["wo",].wait()
    out_core, out_home = {}, {}

    def forward_heads(d):
        for h in range(kv_heads):
            head_group[h, d].wait_recv()
            landed = heads.at[group_from(d), rank, :, head_columns[h]]
            for r in near_ranks:
                head_rank[h, d, r] = go(landed, landed, rank_place(r))

    def project_out(d):
        source = group_from(d)
        for h in range(kv_heads):
            for r in near_ranks:
                head_rank[h, d, r].wait_recv()
        part_out[source] = (
            jnp.dot(
                heads[source].reshape(ranks * span, heads.shape[3]),
                wo[...],
                preferred_element_type=f32,
            )
            .astype(narrow)
            .reshape(ranks, cores, half, out_width)
        )
        out_core[d] = go(part_out.at[source, :, 1 - mdl], near_out.at[source], other)

    def send_out(d):
        source = group_from(d)
        out_core[d].wait_recv()
        for r in every_rank:
            giver = rank_from(r)
            total = part_out[source, giver, mdl].astype(f32) + near_out[source, giver].astype(f32)
            if d or r:
                part_out[source, giver, mdl] = total.astype(narrow)
                out_home[d, r] = go(
                    part_out.at[source, giver, mdl],
                    in_out.at[tok],
                    place(source * ranks + giver, mdl),
                )
            else:
                in_out[tok] = total.astype(narrow)

    for s in range(groups + 2):
        if 0 < s < groups:
            forward_heads(order[s])
        if 0 <= s - 1 < groups:
            project_out(order[s - 1])
        if 0 <= s - 2 < groups:
            send_out(order[s - 2])
    for d in order:
        for r in every_rank:
            if d or r:
                out_home[d, r].wait_recv()
    square = jnp.zeros((half, 1), f32)
    for t in range(toks):
        at = pl.ds(t * depth, depth)
        total = full[:, at].astype(f32) + in_out[t].astype(f32)
        resid[:, at] = total
        square += jnp.sum(total * total, axis=1, keepdims=True)
    row_scale = lax.rsqrt(square * (1.0 / width) + eps_norm)
    all_sent()
    tokens = full
    tokens[...] = (resid[...] * row_scale * moe_gain[...].astype(f32)).astype(narrow)

    main = send.shape[1]
    cap = select.shape[0] // groups
    rest = cap - main
    hidden_units = slab.shape[1]
    packed = cut(send.shape[2], pieces)
    blocks = part // LANES
    main_rows = cores * toks * main
    tile = divide(hidden_units)

    def pack(target, lead, rows_in, row, c):
        for b in range(blocks):
            spot, lane = divmod(b, main // rest)
            at = c * (send.shape[2] // pieces) + part + spot * LANES
            target[(*lead, pl.ds(lane * rest, rest), pl.ds(at, LANES))] = rows_in[
                row : row + rest, b * LANES : (b + 1) * LANES
            ]

    def unpack(target, row, source, lead, c):
        for b in range(blocks):
            spot, lane = divmod(b, main // rest)
            at = c * (send.shape[2] // pieces) + part + spot * LANES
            target[row : row + rest, b * LANES : (b + 1) * LANES] = source[
                (*lead, pl.ds(lane * rest, rest), pl.ds(at, LANES))
            ]

    def body(c):
        return pl.ds(c * (send.shape[2] // pieces), part)

    by_group, by_rank, by_core = {}, {}, {}
    for c in range(pieces):
        picked = jnp.dot(
            select[...], tokens[:, columns[c]], preferred_element_type=jnp.float32
        ).astype(send.dtype)
        for e in range(groups):
            send[e, :, body(c)] = picked[e * main : (e + 1) * main]
            pack(send, (e,), picked, groups * main + e * rest, c)
        for d in far:
            by_group[c, d] = go(
                send.at[(group + d) % groups, :, packed[c]],
                recv.at[mdl, group, rank, :, packed[c]],
                group_place(d),
            )
        for r in near_ranks:
            by_rank[c, 0, r] = go(
                send.at[group, :, packed[c]],
                recv.at[mdl, group, rank, :, packed[c]],
                rank_place(r),
            )
        by_core[c, 0, 0] = go(
            send.at[group, :, packed[c]], recv.at[mdl, group, rank, :, packed[c]], other
        )

    recv[mdl, group, rank] = send[group]

    def from_groups(c):
        for d in far:
            by_group[c, d].wait_recv()
            source = (group + groups - d) % groups
            block = recv.at[mdl, source, rank, :, packed[c]]
            for r in near_ranks:
                by_rank[c, d, r] = go(block, block, rank_place(r))
            by_core[c, d, 0] = go(block, block, other)

    def from_ranks(c):
        for d in [0] + far:
            for r in near_ranks:
                by_rank[c, d, r].wait_recv()
                source = (group + groups - d) % groups
                giver = (rank + ranks - r) % ranks
                block = recv.at[mdl, source, giver, :, packed[c]]
                by_core[c, d, r] = go(block, block, other)

    def assemble(c):
        for d in [0] + far:
            for r in [0] + near_ranks:
                by_core[c, d, r].wait_recv()
        rows[0:main_rows, :] = recv[:, :, :, :, body(c)].reshape(main_rows, part)
        spot = main_rows
        for m in range(cores):
            for g in range(groups):
                for r in range(ranks):
                    unpack(rows, spot, recv, (m, g, r), c)
                    spot += rest

    def project(c):
        assemble(c)
        loads["gate", c].wait()
        loads["up", c].wait()

        def step(n, carry):
            at = pl.ds(pl.multiple_of(n * tile, tile), tile)
            x = rows[...]
            gate_val = jnp.dot(x, gate_w[columns[c], at], preferred_element_type=jnp.float32)
            up_val = jnp.dot(x, up_w[columns[c], at], preferred_element_type=jnp.float32)
            if c > 0:
                gate_val = gate_val + gate_acc[:, at]
                up_val = up_val + up_acc[:, at]
            if c < pieces - 1:
                gate_acc[:, at] = gate_val
                up_acc[:, at] = up_val
            else:
                slab[:, at] = (gate_val / (1.0 + jnp.exp(-gate_val)) * up_val).astype(slab.dtype)
            return carry

        lax.fori_loop(0, hidden_units // tile, step, 0)

    for s in range(pieces + 2):
        if s < pieces:
            from_groups(s)
        if 0 <= s - 1 < pieces:
            from_ranks(s - 1)
        if 0 <= s - 2 < pieces:
            project(s - 2)

    all_sent()
    down_tile = divide(part)
    across, to_rank, to_home = {}, {}, {}

    def down(c):
        loads["down", c].wait()

        def step(n, carry):
            at = pl.multiple_of(n * down_tile, down_tile)
            rows[:, pl.ds(at, down_tile)] = jnp.dot(
                slab[...],
                down_w[c, :, pl.ds(at, down_tile)],
                preferred_element_type=jnp.float32,
            ).astype(rows.dtype)
            return carry

        lax.fori_loop(0, part // down_tile, step, 0)
        recv[:, :, :, :, body(c)] = rows[0:main_rows, :].reshape(cores, groups, ranks, main, part)
        spot = main_rows
        for m in range(cores):
            for g in range(groups):
                for r in range(ranks):
                    pack(recv, (m, g, r), rows, spot, c)
                    spot += rest
        across[c] = go(
            recv.at[1 - mdl, :, :, :, packed[c]], near.at[:, :, :, packed[c]], other
        )

    def pair(g, r, c):
        return recv[mdl, g, r, :, packed[c]].astype(jnp.float32) + near[
            g, r, :, packed[c]
        ].astype(jnp.float32)

    def to_ranks(c):
        across[c].wait_recv()
        for r in near_ranks:
            there = (rank + r) % ranks
            for g in range(groups):
                recv[mdl, g, there, :, packed[c]] = pair(g, there, c).astype(recv.dtype)
            to_rank[c, r] = go(
                recv.at[mdl, :, there, :, packed[c]], mid.at[r - 1, :, :, packed[c]], rank_place(r)
            )

    def to_sources(c):
        for r in near_ranks:
            to_rank[c, r].wait_recv()
        for d in far[::-1] + [0]:
            there = (group + d) % groups
            total = pair(there, rank, c)
            for r in near_ranks:
                total = total + mid[r - 1, there, :, packed[c]].astype(jnp.float32)
            if d == 0:
                home[group, :, packed[c]] = total.astype(home.dtype)
            else:
                recv[mdl, there, rank, :, packed[c]] = total.astype(recv.dtype)
                to_home[c, d] = go(
                    recv.at[mdl, there, rank, :, packed[c]],
                    home.at[group, :, packed[c]],
                    group_place(d),
                )

    def finish(c):
        for d in far:
            to_home[c, d].wait_recv()
        rows[0 : groups * main, :] = home[:, :, body(c)].reshape(groups * main, part)
        for e in range(groups):
            unpack(rows, groups * main + e * rest, home, (e,), c)
        terms = jnp.dot(
            weights[...], rows[0 : groups * cap, :], preferred_element_type=jnp.float32
        )
        total = resid[:, columns[c]]
        for k in range(weights.shape[0] // resid.shape[0]):
            total = total + terms[k * resid.shape[0] : (k + 1) * resid.shape[0]]
        mixed[:, columns[c]] = total.astype(mixed.dtype)

    lag_rank, lag_source, lag_end = 1, 2, 4
    for s in range(pieces + lag_end):
        if s < pieces:
            down(s)
        if 0 <= s - lag_rank < pieces:
            to_ranks(s - lag_rank)
        if 0 <= s - lag_source < pieces:
            to_sources(s - lag_source)
        if 0 <= s - lag_end < pieces:
            finish(s - lag_end)
    all_sent()


def layer(
    dims,
    lengths,
    hidden,
    queries,
    cosines,
    sines,
    attn_gain,
    moe_gain,
    select,
    weights,
    cache,
    wkv,
    wo,
    w_gate,
    w_up,
    w_down,
):
    groups, ranks, cores, pieces = dims
    toks = groups * ranks
    span, features = hidden.shape
    half, width = span // cores, features * cores
    cap = select.shape[0] // groups
    main = cap // 16 * 16
    packed = width // main * cap
    depth, units = w_gate.shape[1:]
    part = width // pieces
    query_heads, _, head_dim = queries.shape
    kv_heads = cache.shape[0]
    query_count = query_heads // kv_heads * span
    kv_width, out_width = wkv.shape[1], wo.shape[1]
    dtype, f32 = hidden.dtype, jnp.float32
    total_rows = cores * toks * cap
    more = max(ranks - 1, 1)
    copies = (
        2
        + (2 * toks - 1)
        + groups * (ranks - 1)
        + groups
        - 1
        + kv_heads * (groups - 1 + groups * (ranks - 1))
        + groups
        + toks
        - 1
        + pieces * ((groups - 1) * 2 + (groups + 1) * (ranks - 1) + toks + 1)
    )
    remote_space = pl.BlockSpec(memory_space=pl.ANY)
    buffers = [
        ((half, width), dtype),
        ((groups, ranks, cores, half, wkv.shape[0]), dtype),
        ((span, head_dim), f32),
        ((span, head_dim), f32),
        ((groups, ranks, span, kv_width), dtype),
        ((more, groups, span, kv_width), dtype),
        ((groups, span, kv_width), dtype),
        ((groups, span, kv_width), dtype),
        (cache.shape, dtype),
        (wkv.shape, dtype),
        (wo.shape, dtype),
        ((kv_heads, query_count, head_dim), f32),
        ((kv_heads, query_count, head_dim), f32),
        ((kv_heads, query_count, head_dim), f32),
        ((groups, ranks, span, wo.shape[0]), dtype),
        ((groups, ranks, cores, half, out_width), dtype),
        ((groups, ranks, half, out_width), dtype),
        ((toks, half, out_width), dtype),
        ((half, width), f32),
        ((groups, main, packed), dtype),
        ((cores, groups, ranks, main, packed), dtype),
        ((groups, ranks, main, packed), dtype),
        ((more, groups, main, packed), dtype),
        ((groups, main, packed), dtype),
        ((total_rows, part), dtype),
        ((depth, units), dtype),
        ((depth, units), dtype),
        ((pieces, units, part), dtype),
        ((total_rows, units), f32),
        ((total_rows, units), f32),
        ((total_rows, units), dtype),
    ]
    return pl.pallas_call(
        functools.partial(layer_kernel, dims),
        out_shape=(
            jax.ShapeDtypeStruct((half, width), dtype),
            jax.ShapeDtypeStruct((span, kv_width), dtype),
        ),
        in_specs=[pl.BlockSpec(memory_space=pltpu.SMEM)] + [VMEM] * 8 + [remote_space] * 6,
        out_specs=(VMEM, VMEM),
        scratch_shapes=[pltpu.VMEM(shape, kind) for shape, kind in buffers]
        + [
            pltpu.SemaphoreType.DMA((2, copies)),
            pltpu.SemaphoreType.DMA((3 * pieces + kv_heads + 2,)),
        ],
        compiler_params=pltpu.CompilerParams(
            collective_id=1, has_side_effects=True, vmem_limit_bytes=67043328
        ),
    )(
        lengths,
        hidden,
        queries,
        cosines,
        sines,
        attn_gain,
        moe_gain,
        select,
        weights,
        cache,
        wkv,
        wo,
        w_gate,
        w_up,
        w_down,
    )


def shards(
    hidden,
    queries,
    cache,
    cache_lengths,
    wkv,
    wo,
    attn_gain,
    moe_gain,
    w_gate,
    w_up,
    w_down,
    expert_ids,
    gates,
):
    span_len = hidden.shape[0]
    toks = lax.axis_size("tok")
    core_count = lax.axis_size("mdl")
    ranks = toks // EXPERTS
    core_rows = span_len // core_count
    kv_heads, _, head_dim = wkv.shape[1:]
    positions = cache_lengths[0] + jnp.arange(span_len, dtype=jnp.int32)
    cosines, sines = rotation(head_dim, positions)
    expert_range = jnp.arange(EXPERTS)
    matches = expert_ids[:, :, None] == expert_range[None, None, :]
    chosen = jnp.sum(matches.astype(jnp.int32), axis=1)
    route = jnp.sum(jnp.where(matches, gates[:, :, None], 0.0), axis=1)
    slot_of = jnp.cumsum(chosen, axis=0) - chosen
    capacity = core_rows * TOPK * 9 // (8 * EXPERTS)
    slot_range = jnp.arange(capacity)
    select = (slot_of.T[:, None, :] == slot_range[None, :, None]) & (chosen.T[:, None, :] > 0)
    main = capacity // 16 * 16

    def by_tile(table):
        return jnp.concatenate(
            [
                table[:, :main].reshape(EXPERTS * main, core_rows),
                table[:, main:].reshape(EXPERTS * (capacity - main), core_rows),
            ]
        )

    picks = by_tile(select.astype(jnp.float32))
    table = by_tile(select.astype(jnp.float32) * route.T[:, None, :]).T
    first = table.astype(jnp.bfloat16)
    second = (table - first.astype(jnp.float32)).astype(jnp.bfloat16)
    third = (table - first.astype(jnp.float32) - second.astype(jnp.float32)).astype(jnp.bfloat16)
    weights = jnp.concatenate([first, second, third])
    mixed, fresh = layer(
        (EXPERTS, ranks, core_count, PIECES),
        cache_lengths,
        hidden,
        queries.transpose(1, 0, 2),
        cosines,
        sines,
        attn_gain[None],
        moe_gain[None],
        picks.astype(jnp.bfloat16),
        weights,
        cache[0].transpose(1, 2, 0, 3),
        wkv.reshape(wkv.shape[0], -1),
        wo.reshape(-1, wo.shape[2]),
        w_gate,
        w_up,
        w_down,
    )
    fresh_key_value = fresh.reshape(span_len, kv_heads, 2, head_dim)
    return (mixed, fresh_key_value)


def solution(mesh):
    in_specs = (
        P(("grp", "tok"), "mdl"),
        P(("grp", "tok"), "mdl", None),
        P(("grp", "tok"), None, "mdl", None, None),
        P(("grp", "tok")),
        P("tok", "mdl", None, None),
        P("mdl", None, "tok"),
        P(),
        P(),
        P(("tok", "mdl"), None, None),
        P(("tok", "mdl"), None, None),
        P(("tok", "mdl"), None, None),
        P(("grp", "tok", "mdl"), None),
        P(("grp", "tok", "mdl"), None),
    )
    out_specs = (P(("grp", "tok", "mdl"), None), P(("grp", "tok"), "mdl", None, None))
    return jax.shard_map(shards, mesh=mesh, in_specs=in_specs, out_specs=out_specs, check_vma=False)
```

```python
import functools
import itertools
import math

import jax
import jax.numpy as jnp
from jax import lax
from jax.experimental import pallas as pl
from jax.experimental.pallas import tpu as pltpu
from jax.sharding import PartitionSpec as P

EXPERTS = 4
TOPK = 2
PIECES = 4


eps_norm = 1e-05
rope_base = 1000000.0
mask_fill = -1e30


def rotation(head_dim, positions):
    half_dim = head_dim // 2
    inverse = jnp.exp(
        jnp.arange(half_dim, dtype=jnp.float32) * (-2.0 * math.log(rope_base) / head_dim)
    )
    angle = positions.astype(jnp.float32)[:, None] * inverse[None, :]
    cosine, sine = jnp.cos(angle), jnp.sin(angle)
    return jnp.concatenate([cosine, cosine], axis=1), jnp.concatenate([-sine, sine], axis=1)


def score_rows(query_rows, key_rows, scale_factor):
    return (
        lax.dot_general(
            query_rows, key_rows, (((1,), (1,)), ((), ())), preferred_element_type=jnp.float32
        )
        * scale_factor
    )


MESH = pl.DeviceIdType.MESH
LANES = 128
VMEM = pl.BlockSpec(memory_space=pltpu.VMEM)


def place(tok, mdl):
    return (lax.axis_index("grp"), tok, mdl)


def greet(peers):
    barrier = pltpu.get_barrier_semaphore()
    for peer in peers:
        pl.semaphore_signal(barrier, inc=1, device_id=peer, device_id_type=MESH)
    pl.semaphore_wait(barrier, len(peers))


def peers_of(groups, ranks, cores):
    tok, mdl = lax.axis_index("tok"), lax.axis_index("mdl")
    group, rank = tok // ranks, tok % ranks
    peers = [place((group + d) % groups * ranks + rank, mdl) for d in range(1, groups)]
    peers += [place(group * ranks + (rank + d) % ranks, mdl) for d in range(1, ranks)]
    if cores:
        peers.append(place(tok, 1 - mdl))
    return peers


def remote(src, dst, sems, index, device):
    copy = pltpu.make_async_remote_copy(
        src_ref=src,
        dst_ref=dst,
        send_sem=sems.at[0, index],
        recv_sem=sems.at[1, index],
        device_id=device,
        device_id_type=MESH,
    )
    copy.start()
    return copy


def near_first(count):
    return sorted(range(1, count), key=lambda d: (min(d, count - d), d))


def cut(width, pieces):
    part = width // pieces
    return [pl.ds(c * part, part) for c in range(pieces)]


def divide(width, choices=(256, 128)):
    for part in choices:
        if width % part == 0 and width // part >= 1:
            return part
    return width


def layer_kernel(
    dims,
    lengths,
    hidden,
    flat_queries,
    cosines,
    sines,
    gains,
    expert_ids,
    gates,
    cache_hbm,
    wkv_hbm,
    wo_hbm,
    gate_hbm,
    up_hbm,
    down_hbm,
    mixed,
    fresh,
    full,
    slices,
    own_square,
    other_square,
    part_kv,
    mid_kv,
    sum_kv,
    in_kv,
    heads,
    part_out,
    near_out,
    in_out,
    resid,
    send,
    recv,
    near,
    mid,
    home,
    gate_w,
    up_w,
    down_w,
    picks,
    weights,
    sems,
    load_sems,
):
    groups, ranks, cores, pieces, kv_heads = dims
    tok, mdl = lax.axis_index("tok"), lax.axis_index("mdl")
    group, rank = tok // ranks, tok % ranks
    toks = groups * ranks
    f32, narrow = jnp.float32, jnp.bfloat16

    width = full.shape[1]
    part = width // pieces
    columns = cut(width, pieces)

    def load(index, src, dst):
        return pltpu.make_async_copy(src, dst, load_sems.at[index])

    def load_gate(c):
        return load(4 + c, gate_hbm.at[0, columns[c], :], gate_w.at[columns[c], :])

    def load_up(c):
        return load(4 + pieces + c, up_hbm.at[0, columns[c], :], up_w.at[columns[c], :])

    def load_down(c):
        return load(4 + 2 * pieces + c, down_hbm.at[0, :, columns[c]], down_w.at[c])

    numbers = itertools.count()
    started = []
    other = place(tok, 1 - mdl)
    far = near_first(groups)
    near_ranks = near_first(ranks)
    every_rank = [0] + near_ranks

    def go(src, dst, device):
        copy = remote(src, dst, sems, next(numbers), device)
        started.append(copy)
        return copy

    def all_sent():
        for copy in started:
            copy.wait_send()
        started.clear()

    def rank_place(r):
        return place(group * ranks + (rank + r) % ranks, mdl)

    def group_place(g):
        return place((group + g) % groups * ranks + rank, mdl)

    def group_from(d):
        return (group + groups - d) % groups

    def rank_from(r):
        return (rank + ranks - r) % ranks

    span, features = hidden.shape
    half = span // cores
    depth = width // toks
    head_dim = flat_queries.shape[1]
    query_heads = flat_queries.shape[0] // span
    per_head = query_heads // kv_heads
    query_count = per_head * span
    limit = cache_hbm.shape[0] // (2 * kv_heads)
    main = send.shape[1]
    cap = picks.shape[0] // groups
    total_rows = cores * toks * cap
    hidden_units = gate_w.shape[1]

    def first_part(*scratch):
        attend(*scratch)
        all_sent()

    def second_part(*scratch):
        mix(*scratch)
        all_sent()


    def mixing(kinds, axis):
        per = LANES // kinds
        down = lax.broadcasted_iota(jnp.int32, (LANES, LANES), 1 - axis)
        along = lax.broadcasted_iota(jnp.int32, (LANES, LANES), axis)
        return jnp.where(along == down % per * kinds + down // per, 1.0, 0.0).astype(narrow)

    def put(ref, kind, at, found):
        ref[kind, at, :] = found

    def sort_rows(flat, kinds, store):
        per = LANES // kinds
        gather = mixing(kinds, 1)
        together = 4
        while flat.shape[0] % (together * LANES):
            together -= 1

        def step(n, carry):
            for b in range(together):
                spot = n * together + b
                taken = flat[pl.ds(pl.multiple_of(spot * LANES, LANES), LANES), :]
                found = jnp.dot(gather, taken, preferred_element_type=f32).astype(narrow)
                at = pl.ds(pl.multiple_of(spot * per, per), per)
                for kind in range(kinds):
                    store(kind, at, found[kind * per : (kind + 1) * per])
            return carry

        lax.fori_loop(0, flat.shape[0] // (together * LANES), step, 0)

    def routes():
        slots = -(-groups * cap // LANES) * LANES
        lane = lax.broadcasted_iota(jnp.int32, (half, slots), 1)
        spare = jnp.maximum(lane - groups * main, 0)
        in_main = lane < groups * main
        expert = jnp.where(in_main, lane // main, spare // (cap - main))
        slot = jnp.where(in_main, lane % main, main + spare % (cap - main))
        chosen = jnp.zeros((half, slots), f32)
        share = jnp.zeros((half, slots), f32)
        for k in range(expert_ids.shape[1]):
            match = expert_ids[:, k : k + 1] == expert
            chosen = chosen + jnp.where(match, 1.0, 0.0)
            share = share + jnp.where(match, gates[:, k : k + 1], 0.0)
        later = lax.broadcasted_iota(jnp.int32, (half, half), 0)
        earlier = lax.broadcasted_iota(jnp.int32, (half, half), 1)
        before = jnp.where(earlier < later, 1.0, 0.0).astype(narrow)
        ahead = jnp.dot(before, chosen.astype(narrow), preferred_element_type=f32)
        real = lane < groups * cap
        pick = jnp.where((ahead == slot.astype(f32)) & real, chosen, 0.0)
        picks[...] = pick.T[: groups * cap].astype(narrow)
        left = pick * share
        for k in range(weights.shape[0] // half):
            term = left.astype(narrow)
            weights[k * half : (k + 1) * half, :] = term[:, : groups * cap]
            left = left - term.astype(f32)

    def attend(flat_cache, flat_wkv, queries, cache, wkv, wo, tops, sums, heads_acc):
        wkv_load = load(0, wkv_hbm, flat_wkv)
        cache_load = load(1, cache_hbm, flat_cache)
        wo_load = load(2, wo_hbm, wo)
        wkv_load.start()
        cache_load.start()
        wo_load.start()
        greet(peers_of(toks, 1, True))


        def lines(core):
            return pl.ds(pl.multiple_of(core * half, half), half)

        def half_features(core):
            return pl.ds(pl.multiple_of(core * features, features), features)

        swap = go(hidden.at[lines(1 - mdl), :], full.at[:, half_features(mdl)], other)
        full[:, half_features(mdl)] = hidden[lines(mdl), :]
        values = hidden[...].astype(f32)
        square = jnp.sum(values * values, axis=1, keepdims=True)
        own_square[...] = jnp.broadcast_to(square, own_square.shape)
        swap_square = go(own_square, other_square, other)
        for c in range(pieces):
            load_gate(c).start()
            load_up(c).start()
        for c in range(pieces):
            load_down(c).start()
        swap.wait_recv()

        def slice_of(target):
            return pl.ds(pl.multiple_of(target * depth, depth), depth)

        outward, twin = {}, {}
        for d in [0] + far:
            for r in every_rank:
                target = (group + d) % groups * ranks + (rank + r) % ranks
                if d or r:
                    outward[d, r] = go(
                        full.at[:, slice_of(target)],
                        slices.at[group, rank, mdl],
                        place(target, mdl),
                    )
        slices[group, rank, mdl] = full[:, slice_of(tok)]
        twin[0, 0] = go(full.at[:, slice_of(tok)], slices.at[group, rank, mdl], other)

        scale_factor = 1.0 / math.sqrt(head_dim)
        block = min(512, limit)

        def query_rows(h):
            return queries[h * per_head : (h + 1) * per_head].reshape(query_count, head_dim)

        def cached_attention(h):
            asked = query_rows(h)
            scores, values = [], []
            for start in range(0, limit, block):
                position = lax.broadcasted_iota(jnp.int32, (query_count, block), 1) + start
                score = score_rows(asked, cache[h, 0, pl.ds(start, block)], scale_factor)
                scores.append(jnp.where(position < lengths[0], score, mask_fill))
                values.append(cache[h, 1, pl.ds(start, block)])
            top = functools.reduce(jnp.maximum, [jnp.max(x, axis=1, keepdims=True) for x in scores])
            total = jnp.zeros((query_count, 1), f32)
            found_values = jnp.zeros((query_count, head_dim), f32)
            for score, value_rows in zip(scores, values):
                chance = jnp.exp(score - top)
                total += jnp.sum(chance, axis=1, keepdims=True)
                found_values += jnp.dot(chance.astype(narrow), value_rows, preferred_element_type=f32)
            tops[h] = jnp.broadcast_to(top, (query_count, head_dim))
            sums[h] = jnp.broadcast_to(total, (query_count, head_dim))
            heads_acc[h] = found_values

        sort_rows(flat_queries, query_heads, lambda kind, at, found: put(queries, kind, at, found))
        cache_load.wait()
        sort_rows(
            flat_cache,
            2 * kv_heads,
            lambda kind, at, found: put(cache.at[kind // 2], kind % 2, at, found),
        )
        wkv_load.wait()

        def put_wkv(kind, at, found):
            wkv[at, kind * head_dim : (kind + 1) * head_dim] = found

        sort_rows(flat_wkv, 2 * kv_heads, put_wkv)
        routes()
        cached_attention(0)

        kv_width = wkv.shape[1]
        gain_rows = depth // LANES
        gain_slice = jnp.concatenate(
            [gains[pl.ds(tok * gain_rows + b, 1), :] for b in range(gain_rows)], axis=1
        )
        kv_rank, kv_home = {}, {}

        def project_kv(d):
            source = group_from(d)
            for r in every_rank:
                if d or r:
                    outward[d, r].wait_recv()
                    landed = slices.at[source, rank_from(r), mdl]
                    twin[d, r] = go(landed, landed, other)
            for r in every_rank:
                twin[d, r].wait_recv()
            taken = slices[source].reshape(ranks * span, depth).astype(f32) * gain_slice
            part_kv[source] = (
                jnp.dot(taken.astype(narrow), wkv[...], preferred_element_type=f32)
                .astype(narrow)
                .reshape(ranks, span, kv_width)
            )
            for r in near_ranks:
                kv_rank[d, r] = go(
                    part_kv.at[source, (rank + r) % ranks], mid_kv.at[r - 1, source], rank_place(r)
                )

        def reduce_kv(d):
            source = group_from(d)
            total = part_kv[source, rank].astype(f32)
            for r in near_ranks:
                kv_rank[d, r].wait_recv()
                total = total + mid_kv[r - 1, source].astype(f32)
            if d:
                sum_kv[source] = total.astype(narrow)
                kv_home[d] = go(sum_kv.at[source], in_kv.at[group], group_place(-d))
            else:
                in_kv[group] = total.astype(narrow)

        order = [0] + far
        for s in range(groups + 1):
            if s < groups:
                project_kv(order[s])
            if s > 0:
                reduce_kv(order[s - 1])
        for h in range(1, kv_heads):
            cached_attention(h)
        swap_square.wait_recv()
        meansq = (own_square[...] + other_square[...]) * (1.0 / width)
        row_scale = lax.rsqrt(meansq + eps_norm)
        for d in far:
            kv_home[d].wait_recv()

        token = lax.broadcasted_iota(jnp.int32, (query_count, span), 0) % span
        column = lax.broadcasted_iota(jnp.int32, (query_count, span), 1)
        head_width = per_head * head_dim
        head_columns = [pl.ds(h * head_width, head_width) for h in range(kv_heads)]
        head_group, head_rank = {}, {}
        new_rows = []
        for h in range(kv_heads):
            pair_of = []
            for kind in range(2):
                at = pl.ds((2 * h + kind) * head_dim, head_dim)
                total = in_kv[0, :, at].astype(f32)
                for g in range(1, groups):
                    total = total + in_kv[g, :, at].astype(f32)
                total = total * row_scale
                if kind == 0:
                    total = total * cosines[...] + pltpu.roll(total, head_dim // 2, 1) * sines[...]
                pair_of.append(total.astype(narrow))
                new_rows.append(pair_of[kind])
            score = score_rows(query_rows(h), pair_of[0], scale_factor)
            score = jnp.where(column <= token, score, mask_fill)
            before = tops[h]
            top = jnp.maximum(before, jnp.max(score, axis=1, keepdims=True))
            fade = jnp.exp(before - top)
            chance = jnp.exp(score - top[:, :1])
            total = sums[h] * fade + jnp.sum(chance, axis=1, keepdims=True)
            attended = heads_acc[h] * fade + jnp.dot(
                chance.astype(narrow), pair_of[1], preferred_element_type=f32
            )
            attended = (attended / total).astype(narrow)
            for head in range(per_head):
                at = pl.ds(h * head_width + head * head_dim, head_dim)
                heads[group, rank, :, at] = attended[head * span : (head + 1) * span]
            own = heads.at[group, rank, :, head_columns[h]]
            for d in far:
                head_group[h, d] = go(own, own, group_place(d))
            for r in near_ranks:
                head_rank[h, 0, r] = go(own, own, rank_place(r))

        kinds = 2 * kv_heads
        step_rows = LANES // kinds
        spread_out = mixing(kinds, 0)
        for b in range(span // step_rows):
            stack = jnp.concatenate(
                [x[b * step_rows : (b + 1) * step_rows] for x in new_rows], axis=0
            )
            fresh[b * LANES : (b + 1) * LANES, :] = jnp.dot(
                spread_out, stack, preferred_element_type=f32
            ).astype(narrow)
        out_width = wo.shape[1]
        wo_load.wait()
        out_core, out_home = {}, {}

        def forward_heads(d):
            for h in range(kv_heads):
                head_group[h, d].wait_recv()
                landed = heads.at[group_from(d), rank, :, head_columns[h]]
                for r in near_ranks:
                    head_rank[h, d, r] = go(landed, landed, rank_place(r))

        def project_out(d):
            source = group_from(d)
            for h in range(kv_heads):
                for r in near_ranks:
                    head_rank[h, d, r].wait_recv()
            part_out[source] = (
                jnp.dot(
                    heads[source].reshape(ranks * span, heads.shape[3]),
                    wo[...],
                    preferred_element_type=f32,
                )
                .astype(narrow)
                .reshape(ranks, cores, half, out_width)
            )
            out_core[d] = go(part_out.at[source, :, 1 - mdl], near_out.at[source], other)

        def send_out(d):
            source = group_from(d)
            out_core[d].wait_recv()
            for r in every_rank:
                giver = rank_from(r)
                total = part_out[source, giver, mdl].astype(f32) + near_out[source, giver].astype(f32)
                if d or r:
                    part_out[source, giver, mdl] = total.astype(narrow)
                    out_home[d, r] = go(
                        part_out.at[source, giver, mdl],
                        in_out.at[tok],
                        place(source * ranks + giver, mdl),
                    )
                else:
                    in_out[tok] = total.astype(narrow)

        for s in range(groups + 2):
            if 0 < s < groups:
                forward_heads(order[s])
            if 0 <= s - 1 < groups:
                project_out(order[s - 1])
            if 0 <= s - 2 < groups:
                send_out(order[s - 2])
        for d in order:
            for r in every_rank:
                if d or r:
                    out_home[d, r].wait_recv()
        square = jnp.zeros((half, 1), f32)
        for t in range(toks):
            at = pl.ds(t * depth, depth)
            total = full[:, at].astype(f32) + in_out[t].astype(f32)
            resid[:, at] = total
            square += jnp.sum(total * total, axis=1, keepdims=True)
        row_scale = lax.rsqrt(square * (1.0 / width) + eps_norm)
        all_sent()
        for b in range(width // LANES):
            at = pl.ds(b * LANES, LANES)
            gain = gains[width // LANES + b : width // LANES + b + 1, :]
            full[:, at] = (resid[:, at] * row_scale * gain).astype(narrow)

    def mix(rows, gate_acc, up_acc, slab):
        tokens = full
        rest = cap - main
        packed = cut(send.shape[2], pieces)
        blocks = part // LANES
        main_rows = cores * toks * main
        tile = divide(hidden_units)

        def pack(target, lead, rows_in, row, c):
            for b in range(blocks):
                spot, lane = divmod(b, main // rest)
                at = c * (send.shape[2] // pieces) + part + spot * LANES
                target[(*lead, pl.ds(lane * rest, rest), pl.ds(at, LANES))] = rows_in[
                    row : row + rest, b * LANES : (b + 1) * LANES
                ]

        def unpack(target, row, source, lead, c):
            for b in range(blocks):
                spot, lane = divmod(b, main // rest)
                at = c * (send.shape[2] // pieces) + part + spot * LANES
                target[row : row + rest, b * LANES : (b + 1) * LANES] = source[
                    (*lead, pl.ds(lane * rest, rest), pl.ds(at, LANES))
                ]

        def body(c):
            return pl.ds(c * (send.shape[2] // pieces), part)

        by_group, by_rank, by_core = {}, {}, {}
        for c in range(pieces):
            picked = jnp.dot(
                picks[...], tokens[:, columns[c]], preferred_element_type=jnp.float32
            ).astype(send.dtype)
            for e in range(groups):
                send[e, :, body(c)] = picked[e * main : (e + 1) * main]
                pack(send, (e,), picked, groups * main + e * rest, c)
            for d in far:
                by_group[c, d] = go(
                    send.at[(group + d) % groups, :, packed[c]],
                    recv.at[mdl, group, rank, :, packed[c]],
                    group_place(d),
                )
            for r in near_ranks:
                by_rank[c, 0, r] = go(
                    send.at[group, :, packed[c]],
                    recv.at[mdl, group, rank, :, packed[c]],
                    rank_place(r),
                )
            by_core[c, 0, 0] = go(
                send.at[group, :, packed[c]], recv.at[mdl, group, rank, :, packed[c]], other
            )

        recv[mdl, group, rank] = send[group]

        def from_groups(c):
            for d in far:
                by_group[c, d].wait_recv()
                source = (group + groups - d) % groups
                block = recv.at[mdl, source, rank, :, packed[c]]
                for r in near_ranks:
                    by_rank[c, d, r] = go(block, block, rank_place(r))
                by_core[c, d, 0] = go(block, block, other)

        def from_ranks(c):
            for d in [0] + far:
                for r in near_ranks:
                    by_rank[c, d, r].wait_recv()
                    source = (group + groups - d) % groups
                    giver = (rank + ranks - r) % ranks
                    block = recv.at[mdl, source, giver, :, packed[c]]
                    by_core[c, d, r] = go(block, block, other)

        def assemble(c):
            for d in [0] + far:
                for r in [0] + near_ranks:
                    by_core[c, d, r].wait_recv()
            rows[0:main_rows, :] = recv[:, :, :, :, body(c)].reshape(main_rows, part)
            spot = main_rows
            for m in range(cores):
                for g in range(groups):
                    for r in range(ranks):
                        unpack(rows, spot, recv, (m, g, r), c)
                        spot += rest

        def project(c):
            assemble(c)
            load_gate(c).wait()
            load_up(c).wait()

            def step(n, carry):
                at = pl.ds(pl.multiple_of(n * tile, tile), tile)
                x = rows[...]
                gate_val = jnp.dot(x, gate_w[columns[c], at], preferred_element_type=jnp.float32)
                up_val = jnp.dot(x, up_w[columns[c], at], preferred_element_type=jnp.float32)
                if c > 0:
                    gate_val = gate_val + gate_acc[:, at]
                    up_val = up_val + up_acc[:, at]
                if c < pieces - 1:
                    gate_acc[:, at] = gate_val
                    up_acc[:, at] = up_val
                else:
                    slab[:, at] = (gate_val / (1.0 + jnp.exp(-gate_val)) * up_val).astype(slab.dtype)
                return carry

            lax.fori_loop(0, hidden_units // tile, step, 0)

        for s in range(pieces + 2):
            if s < pieces:
                from_groups(s)
            if 0 <= s - 1 < pieces:
                from_ranks(s - 1)
            if 0 <= s - 2 < pieces:
                project(s - 2)

        all_sent()
        down_tile = divide(part)
        across, to_rank, to_home = {}, {}, {}

        def down(c):
            load_down(c).wait()

            def step(n, carry):
                at = pl.multiple_of(n * down_tile, down_tile)
                rows[:, pl.ds(at, down_tile)] = jnp.dot(
                    slab[...],
                    down_w[c, :, pl.ds(at, down_tile)],
                    preferred_element_type=jnp.float32,
                ).astype(rows.dtype)
                return carry

            lax.fori_loop(0, part // down_tile, step, 0)
            recv[:, :, :, :, body(c)] = rows[0:main_rows, :].reshape(cores, groups, ranks, main, part)
            spot = main_rows
            for m in range(cores):
                for g in range(groups):
                    for r in range(ranks):
                        pack(recv, (m, g, r), rows, spot, c)
                        spot += rest
            across[c] = go(
                recv.at[1 - mdl, :, :, :, packed[c]], near.at[:, :, :, packed[c]], other
            )

        def pair(g, r, c):
            return recv[mdl, g, r, :, packed[c]].astype(jnp.float32) + near[
                g, r, :, packed[c]
            ].astype(jnp.float32)

        def to_ranks(c):
            across[c].wait_recv()
            for r in near_ranks:
                there = (rank + r) % ranks
                for g in range(groups):
                    recv[mdl, g, there, :, packed[c]] = pair(g, there, c).astype(recv.dtype)
                to_rank[c, r] = go(
                    recv.at[mdl, :, there, :, packed[c]], mid.at[r - 1, :, :, packed[c]], rank_place(r)
                )

        def to_sources(c):
            for r in near_ranks:
                to_rank[c, r].wait_recv()
            for d in far[::-1] + [0]:
                there = (group + d) % groups
                total = pair(there, rank, c)
                for r in near_ranks:
                    total = total + mid[r - 1, there, :, packed[c]].astype(jnp.float32)
                if d == 0:
                    home[group, :, packed[c]] = total.astype(home.dtype)
                else:
                    recv[mdl, there, rank, :, packed[c]] = total.astype(recv.dtype)
                    to_home[c, d] = go(
                        recv.at[mdl, there, rank, :, packed[c]],
                        home.at[group, :, packed[c]],
                        group_place(d),
                    )

        def finish(c):
            for d in far:
                to_home[c, d].wait_recv()
            rows[0 : groups * main, :] = home[:, :, body(c)].reshape(groups * main, part)
            for e in range(groups):
                unpack(rows, groups * main + e * rest, home, (e,), c)
            terms = jnp.dot(
                weights[...], rows[0 : groups * cap, :], preferred_element_type=jnp.float32
            )
            total = resid[:, columns[c]]
            for k in range(weights.shape[0] // resid.shape[0]):
                total = total + terms[k * resid.shape[0] : (k + 1) * resid.shape[0]]
            mixed[:, columns[c]] = total.astype(mixed.dtype)

        lag_rank, lag_source, lag_end = 1, 2, 4
        for s in range(pieces + lag_end):
            if s < pieces:
                down(s)
            if 0 <= s - lag_rank < pieces:
                to_ranks(s - lag_rank)
            if 0 <= s - lag_source < pieces:
                to_sources(s - lag_source)
            if 0 <= s - lag_end < pieces:
                finish(s - lag_end)

    scoped = [
        (cache_hbm.shape, narrow),
        (wkv_hbm.shape, narrow),
        ((query_heads, span, head_dim), narrow),
        ((kv_heads, 2, limit, head_dim), narrow),
        ((depth, 2 * kv_heads * head_dim), narrow),
        (wo_hbm.shape, narrow),
        ((kv_heads, query_count, head_dim), f32),
        ((kv_heads, query_count, head_dim), f32),
        ((kv_heads, query_count, head_dim), f32),
    ]
    pl.run_scoped(first_part, *[pltpu.VMEM(shape, kind) for shape, kind in scoped])
    scoped = [
        ((total_rows, part), narrow),
        ((total_rows, hidden_units), f32),
        ((total_rows, hidden_units), f32),
        ((total_rows, hidden_units), narrow),
    ]
    pl.run_scoped(second_part, *[pltpu.VMEM(shape, kind) for shape, kind in scoped])


def layer(
    dims,
    lengths,
    hidden,
    queries,
    cosines,
    sines,
    gains,
    expert_ids,
    gates,
    cache,
    wkv,
    wo,
    w_gate,
    w_up,
    w_down,
):
    groups, ranks, cores, pieces, kv_heads = dims
    toks = groups * ranks
    span, features = hidden.shape
    half, width = span // cores, features * cores
    cap = half * TOPK * 9 // (8 * groups)
    main = cap // 16 * 16
    packed = width // main * cap
    depth, units = w_gate.shape[1:]
    part = width // pieces
    head_dim = queries.shape[1]
    kv_width, out_width = 2 * kv_heads * head_dim, wo.shape[1]
    depth_slice = width // toks
    dtype, f32 = hidden.dtype, jnp.float32
    more = max(ranks - 1, 1)
    copies = (
        2
        + (2 * toks - 1)
        + groups * (ranks - 1)
        + groups
        - 1
        + kv_heads * (groups - 1 + groups * (ranks - 1))
        + groups
        + toks
        - 1
        + pieces * ((groups - 1) * 2 + (groups + 1) * (ranks - 1) + toks + 1)
    )
    remote_space = pl.BlockSpec(memory_space=pl.ANY)
    buffers = [
        ((half, width), dtype),
        ((groups, ranks, cores, half, depth_slice), dtype),
        ((span, head_dim), f32),
        ((span, head_dim), f32),
        ((groups, ranks, span, kv_width), dtype),
        ((more, groups, span, kv_width), dtype),
        ((groups, span, kv_width), dtype),
        ((groups, span, kv_width), dtype),
        ((groups, ranks, span, wo.shape[0]), dtype),
        ((groups, ranks, cores, half, out_width), dtype),
        ((groups, ranks, half, out_width), dtype),
        ((toks, half, out_width), dtype),
        ((half, width), f32),
        ((groups, main, packed), dtype),
        ((cores, groups, ranks, main, packed), dtype),
        ((groups, ranks, main, packed), dtype),
        ((more, groups, main, packed), dtype),
        ((groups, main, packed), dtype),
        ((depth, units), dtype),
        ((depth, units), dtype),
        ((pieces, units, part), dtype),
        ((groups * cap, half), dtype),
        ((3 * half, groups * cap), dtype),
    ]
    return pl.pallas_call(
        functools.partial(layer_kernel, dims),
        out_shape=(
            jax.ShapeDtypeStruct((half, width), dtype),
            jax.ShapeDtypeStruct((span * 2 * kv_heads, head_dim), dtype),
        ),
        in_specs=[pl.BlockSpec(memory_space=pltpu.SMEM)] + [VMEM] * 7 + [remote_space] * 6,
        out_specs=(VMEM, VMEM),
        scratch_shapes=[pltpu.VMEM(shape, kind) for shape, kind in buffers]
        + [
            pltpu.SemaphoreType.DMA((2, copies)),
            pltpu.SemaphoreType.DMA((3 * pieces + 4,)),
        ],
        compiler_params=pltpu.CompilerParams(
            collective_id=1, has_side_effects=True, vmem_limit_bytes=67043328
        ),
    )(
        lengths,
        hidden,
        queries,
        cosines,
        sines,
        gains,
        expert_ids,
        gates,
        cache,
        wkv,
        wo,
        w_gate,
        w_up,
        w_down,
    )


def shards(
    hidden,
    queries,
    cache,
    cache_lengths,
    wkv,
    wo,
    attn_gain,
    moe_gain,
    w_gate,
    w_up,
    w_down,
    expert_ids,
    gates,
):
    span_len = hidden.shape[0]
    toks = lax.axis_size("tok")
    core_count = lax.axis_size("mdl")
    ranks = toks // EXPERTS
    kv_heads, _, head_dim = wkv.shape[1:]
    positions = cache_lengths[0] + jnp.arange(span_len, dtype=jnp.int32)
    cosines, sines = rotation(head_dim, positions)
    gains = jnp.concatenate([attn_gain, moe_gain]).astype(jnp.float32).reshape(-1, LANES)
    mixed, fresh = layer(
        (EXPERTS, ranks, core_count, PIECES, kv_heads),
        cache_lengths,
        hidden,
        queries.reshape(-1, head_dim),
        cosines,
        sines,
        gains,
        expert_ids,
        gates,
        cache.reshape(-1, head_dim),
        wkv.reshape(-1, head_dim),
        wo.reshape(-1, wo.shape[2]),
        w_gate,
        w_up,
        w_down,
    )
    fresh_key_value = fresh.reshape(span_len, kv_heads, 2, head_dim)
    return (mixed, fresh_key_value)


def solution(mesh):
    in_specs = (
        P(("grp", "tok"), "mdl"),
        P(("grp", "tok"), "mdl", None),
        P(("grp", "tok"), None, "mdl", None, None),
        P(("grp", "tok")),
        P("tok", "mdl", None, None),
        P("mdl", None, "tok"),
        P(),
        P(),
        P(("tok", "mdl"), None, None),
        P(("tok", "mdl"), None, None),
        P(("tok", "mdl"), None, None),
        P(("grp", "tok", "mdl"), None),
        P(("grp", "tok", "mdl"), None),
    )
    out_specs = (P(("grp", "tok", "mdl"), None), P(("grp", "tok"), "mdl", None, None))
    return jax.shard_map(shards, mesh=mesh, in_specs=in_specs, out_specs=out_specs, check_vma=False)
```

```python
import functools
import itertools
import math

import jax
import jax.numpy as jnp
from jax import lax
from jax.experimental import pallas as pl
from jax.experimental.pallas import tpu as pltpu
from jax.sharding import PartitionSpec as P

EXPERTS = 4
TOPK = 2
PIECES = 4


eps_norm = 1e-05
rope_base = 1000000.0
mask_fill = -1e30


def rotation(head_dim, positions):
    half_dim = head_dim // 2
    inverse = jnp.exp(
        jnp.arange(half_dim, dtype=jnp.float32) * (-2.0 * math.log(rope_base) / head_dim)
    )
    angle = positions.astype(jnp.float32)[:, None] * inverse[None, :]
    cosine, sine = jnp.cos(angle), jnp.sin(angle)
    return cosine, sine


def score_rows(query_rows, key_rows, scale_factor):
    return (
        lax.dot_general(
            query_rows, key_rows, (((1,), (1,)), ((), ())), preferred_element_type=jnp.float32
        )
        * scale_factor
    )


MESH = pl.DeviceIdType.MESH
LANES = 128
VMEM = pl.BlockSpec(memory_space=pltpu.VMEM)


def place(tok, mdl):
    return (lax.axis_index("grp"), tok, mdl)


def greet(peers):
    barrier = pltpu.get_barrier_semaphore()
    for peer in peers:
        pl.semaphore_signal(barrier, inc=1, device_id=peer, device_id_type=MESH)
    pl.semaphore_wait(barrier, len(peers))


def peers_of(groups, ranks, cores):
    tok, mdl = lax.axis_index("tok"), lax.axis_index("mdl")
    group, rank = tok // ranks, tok % ranks
    peers = [place((group + d) % groups * ranks + rank, mdl) for d in range(1, groups)]
    peers += [place(group * ranks + (rank + d) % ranks, mdl) for d in range(1, ranks)]
    if cores:
        peers.append(place(tok, 1 - mdl))
    return peers


def remote(src, dst, sems, index, device):
    copy = pltpu.make_async_remote_copy(
        src_ref=src,
        dst_ref=dst,
        send_sem=sems.at[0, index],
        recv_sem=sems.at[1, index],
        device_id=device,
        device_id_type=MESH,
    )
    copy.start()
    return copy


def near_first(count):
    return sorted(range(1, count), key=lambda d: (min(d, count - d), d))


def cut(width, pieces):
    part = width // pieces
    return [pl.ds(c * part, part) for c in range(pieces)]


def divide(width, choices=(256, 128)):
    for part in choices:
        if width % part == 0 and width // part >= 1:
            return part
    return width


def layer_kernel(
    dims,
    lengths,
    hidden,
    flat_queries,
    cosines,
    sines,
    gains,
    cache_hbm,
    wkv_hbm,
    wo_hbm,
    gate_hbm,
    up_hbm,
    down_hbm,
    mixed,
    fresh,
    full,
    slices,
    own_square,
    other_square,
    part_kv,
    mid_kv,
    sum_kv,
    in_kv,
    heads,
    part_out,
    near_out,
    in_out,
    resid,
    send,
    recv,
    near,
    mid,
    home,
    gate_w,
    up_w,
    down_w,
    picks,
    weights,
    sems,
    load_sems,
):
    groups, ranks, cores, pieces, kv_heads = dims
    tok, mdl = lax.axis_index("tok"), lax.axis_index("mdl")
    group, rank = tok // ranks, tok % ranks
    toks = groups * ranks
    f32, narrow = jnp.float32, jnp.bfloat16

    width = full.shape[1]
    part = width // pieces
    columns = cut(width, pieces)

    def load(index, src, dst):
        return pltpu.make_async_copy(src, dst, load_sems.at[index])

    def load_gate(c):
        return load(4 + c, gate_hbm.at[0, columns[c], :], gate_w.at[columns[c], :])

    def load_up(c):
        return load(4 + pieces + c, up_hbm.at[0, columns[c], :], up_w.at[columns[c], :])

    def load_down(c):
        return load(4 + 2 * pieces + c, down_hbm.at[0, :, columns[c]], down_w.at[c])

    numbers = itertools.count()
    started = []
    other = place(tok, 1 - mdl)
    far = near_first(groups)
    near_ranks = near_first(ranks)
    every_rank = [0] + near_ranks

    def go(src, dst, device):
        copy = remote(src, dst, sems, next(numbers), device)
        started.append(copy)
        return copy

    def all_sent():
        for copy in started:
            copy.wait_send()
        started.clear()

    def rank_place(r):
        return place(group * ranks + (rank + r) % ranks, mdl)

    def group_place(g):
        return place((group + g) % groups * ranks + rank, mdl)

    def group_from(d):
        return (group + groups - d) % groups

    def rank_from(r):
        return (rank + ranks - r) % ranks

    span, features = hidden.shape
    half = span // cores
    depth = width // toks
    head_dim = flat_queries.shape[1]
    query_heads = flat_queries.shape[0] // span
    per_head = query_heads // kv_heads
    query_count = per_head * span
    limit = cache_hbm.shape[0] // (2 * kv_heads)
    main = send.shape[1]
    cap = picks.shape[0] // groups
    total_rows = cores * toks * cap
    hidden_units = gate_w.shape[1]

    def first_part(*scratch):
        attend(*scratch)
        all_sent()

    def second_part(*scratch):
        mix(*scratch)
        all_sent()


    def mixing(kinds, axis):
        per = LANES // kinds
        down = lax.broadcasted_iota(jnp.int32, (LANES, LANES), 1 - axis)
        along = lax.broadcasted_iota(jnp.int32, (LANES, LANES), axis)
        return jnp.where(along == down % per * kinds + down // per, 1.0, 0.0).astype(narrow)

    def put(ref, kind, at, found):
        ref[kind, at, :] = found

    def sort_rows(flat, kinds, store):
        per = LANES // kinds
        gather = mixing(kinds, 1)
        together = 4
        while flat.shape[0] % (together * LANES):
            together -= 1

        def step(n, carry):
            for b in range(together):
                spot = n * together + b
                taken = flat[pl.ds(pl.multiple_of(spot * LANES, LANES), LANES), :]
                found = jnp.dot(gather, taken, preferred_element_type=f32).astype(narrow)
                at = pl.ds(pl.multiple_of(spot * per, per), per)
                for kind in range(kinds):
                    store(kind, at, found[kind * per : (kind + 1) * per])
            return carry

        lax.fori_loop(0, flat.shape[0] // (together * LANES), step, 0)

    def routes():
        slots = -(-groups * cap // LANES) * LANES
        lane = lax.broadcasted_iota(jnp.int32, (half, slots), 1)
        spare = jnp.maximum(lane - groups * main, 0)
        in_main = lane < groups * main
        expert = jnp.where(in_main, lane // main, spare // (cap - main))
        slot = jnp.where(in_main, lane % main, main + spare % (cap - main))
        chosen = jnp.zeros((half, slots), f32)
        share = jnp.zeros((half, slots), f32)
        named = gains[gains.shape[0] - half :, :]
        for k in range(TOPK):
            match = named[:, k : k + 1] == expert.astype(f32)
            chosen = chosen + jnp.where(match, 1.0, 0.0)
            share = share + jnp.where(match, named[:, TOPK + k : TOPK + k + 1], 0.0)
        later = lax.broadcasted_iota(jnp.int32, (half, half), 0)
        earlier = lax.broadcasted_iota(jnp.int32, (half, half), 1)
        before = jnp.where(earlier < later, 1.0, 0.0).astype(narrow)
        ahead = jnp.dot(before, chosen.astype(narrow), preferred_element_type=f32)
        real = lane < groups * cap
        pick = jnp.where((ahead == slot.astype(f32)) & real, chosen, 0.0)
        picks[...] = pick.T[: groups * cap].astype(narrow)
        left = pick * share
        for k in range(weights.shape[0] // half):
            term = left.astype(narrow)
            weights[k * half : (k + 1) * half, :] = term[:, : groups * cap]
            left = left - term.astype(f32)

    def attend(flat_cache, flat_wkv, queries, cache, wkv, wo, tops, sums, heads_acc):
        wkv_load = load(0, wkv_hbm, flat_wkv)
        cache_load = load(1, cache_hbm, flat_cache)
        wo_load = load(2, wo_hbm, wo)
        wkv_load.start()
        cache_load.start()
        wo_load.start()
        greet(peers_of(toks, 1, True))


        def lines(core):
            return pl.ds(pl.multiple_of(core * half, half), half)

        def half_features(core):
            return pl.ds(pl.multiple_of(core * features, features), features)

        swap = go(hidden.at[lines(1 - mdl), :], full.at[:, half_features(mdl)], other)
        full[:, half_features(mdl)] = hidden[lines(mdl), :]
        values = hidden[...].astype(f32)
        square = jnp.sum(values * values, axis=1, keepdims=True)
        own_square[...] = jnp.broadcast_to(square, own_square.shape)
        swap_square = go(own_square, other_square, other)
        for c in range(pieces):
            load_gate(c).start()
            load_up(c).start()
        for c in range(pieces):
            load_down(c).start()
        swap.wait_recv()

        def slice_of(target):
            return pl.ds(pl.multiple_of(target * depth, depth), depth)

        outward, twin = {}, {}
        for d in [0] + far:
            for r in every_rank:
                target = (group + d) % groups * ranks + (rank + r) % ranks
                if d or r:
                    outward[d, r] = go(
                        full.at[:, slice_of(target)],
                        slices.at[group, rank, mdl],
                        place(target, mdl),
                    )
        slices[group, rank, mdl] = full[:, slice_of(tok)]
        twin[0, 0] = go(full.at[:, slice_of(tok)], slices.at[group, rank, mdl], other)

        scale_factor = 1.0 / math.sqrt(head_dim)
        block = min(512, limit)

        def query_rows(h):
            return queries[h * per_head : (h + 1) * per_head].reshape(query_count, head_dim)

        def cached_attention(h):
            asked = query_rows(h)
            scores, values = [], []
            for start in range(0, limit, block):
                position = lax.broadcasted_iota(jnp.int32, (query_count, block), 1) + start
                score = score_rows(asked, cache[h, 0, pl.ds(start, block)], scale_factor)
                scores.append(jnp.where(position < lengths[0], score, mask_fill))
                values.append(cache[h, 1, pl.ds(start, block)])
            top = functools.reduce(jnp.maximum, [jnp.max(x, axis=1, keepdims=True) for x in scores])
            total = jnp.zeros((query_count, 1), f32)
            found_values = jnp.zeros((query_count, head_dim), f32)
            for score, value_rows in zip(scores, values):
                chance = jnp.exp(score - top)
                total += jnp.sum(chance, axis=1, keepdims=True)
                found_values += jnp.dot(chance.astype(narrow), value_rows, preferred_element_type=f32)
            tops[h] = jnp.broadcast_to(top, (query_count, head_dim))
            sums[h] = jnp.broadcast_to(total, (query_count, head_dim))
            heads_acc[h] = found_values

        sort_rows(flat_queries, query_heads, lambda kind, at, found: put(queries, kind, at, found))
        cache_load.wait()
        sort_rows(
            flat_cache,
            2 * kv_heads,
            lambda kind, at, found: put(cache.at[kind // 2], kind % 2, at, found),
        )
        wkv_load.wait()

        def put_wkv(kind, at, found):
            wkv[at, kind * head_dim : (kind + 1) * head_dim] = found

        sort_rows(flat_wkv, 2 * kv_heads, put_wkv)

        kv_width = wkv.shape[1]
        gain_rows = depth // LANES
        gain_slice = jnp.concatenate(
            [gains[pl.ds(tok * gain_rows + b, 1), :] for b in range(gain_rows)], axis=1
        )
        kv_rank, kv_home = {}, {}

        def project_kv(d):
            source = group_from(d)
            for r in every_rank:
                if d or r:
                    outward[d, r].wait_recv()
                    landed = slices.at[source, rank_from(r), mdl]
                    twin[d, r] = go(landed, landed, other)
            for r in every_rank:
                twin[d, r].wait_recv()
            taken = slices[source].reshape(ranks * span, depth).astype(f32) * gain_slice
            part_kv[source] = (
                jnp.dot(taken.astype(narrow), wkv[...], preferred_element_type=f32)
                .astype(narrow)
                .reshape(ranks, span, kv_width)
            )
            for r in near_ranks:
                kv_rank[d, r] = go(
                    part_kv.at[source, (rank + r) % ranks], mid_kv.at[r - 1, source], rank_place(r)
                )

        def reduce_kv(d):
            source = group_from(d)
            total = part_kv[source, rank].astype(f32)
            for r in near_ranks:
                kv_rank[d, r].wait_recv()
                total = total + mid_kv[r - 1, source].astype(f32)
            if d:
                sum_kv[source] = total.astype(narrow)
                kv_home[d] = go(sum_kv.at[source], in_kv.at[group], group_place(-d))
            else:
                in_kv[group] = total.astype(narrow)

        order = [0] + far
        for s in range(groups + 1):
            if s < groups:
                project_kv(order[s])
            if s > 0:
                reduce_kv(order[s - 1])
        for h in range(kv_heads):
            cached_attention(h)
        swap_square.wait_recv()
        meansq = (own_square[...] + other_square[...]) * (1.0 / width)
        row_scale = lax.rsqrt(meansq + eps_norm)
        for d in far:
            kv_home[d].wait_recv()

        token = lax.broadcasted_iota(jnp.int32, (query_count, span), 0) % span
        column = lax.broadcasted_iota(jnp.int32, (query_count, span), 1)
        head_width = per_head * head_dim
        head_columns = [pl.ds(h * head_width, head_width) for h in range(kv_heads)]
        turn = jnp.concatenate([cosines[...], cosines[...]], axis=1)
        shift = jnp.concatenate([-sines[...], sines[...]], axis=1)
        head_group, head_rank = {}, {}
        new_rows = []
        for h in range(kv_heads):
            pair_of = []
            for kind in range(2):
                at = pl.ds((2 * h + kind) * head_dim, head_dim)
                total = in_kv[0, :, at].astype(f32)
                for g in range(1, groups):
                    total = total + in_kv[g, :, at].astype(f32)
                total = total * row_scale
                if kind == 0:
                    total = total * turn + pltpu.roll(total, head_dim // 2, 1) * shift
                pair_of.append(total.astype(narrow))
                new_rows.append(pair_of[kind])
            score = score_rows(query_rows(h), pair_of[0], scale_factor)
            score = jnp.where(column <= token, score, mask_fill)
            before = tops[h]
            top = jnp.maximum(before, jnp.max(score, axis=1, keepdims=True))
            fade = jnp.exp(before - top)
            chance = jnp.exp(score - top[:, :1])
            total = sums[h] * fade + jnp.sum(chance, axis=1, keepdims=True)
            attended = heads_acc[h] * fade + jnp.dot(
                chance.astype(narrow), pair_of[1], preferred_element_type=f32
            )
            attended = (attended / total).astype(narrow)
            for head in range(per_head):
                at = pl.ds(h * head_width + head * head_dim, head_dim)
                heads[group, rank, :, at] = attended[head * span : (head + 1) * span]
            own = heads.at[group, rank, :, head_columns[h]]
            for d in far:
                head_group[h, d] = go(own, own, group_place(d))
            for r in near_ranks:
                head_rank[h, 0, r] = go(own, own, rank_place(r))

        kinds = 2 * kv_heads
        step_rows = LANES // kinds
        spread_out = mixing(kinds, 0)
        for b in range(span // step_rows):
            stack = jnp.concatenate(
                [x[b * step_rows : (b + 1) * step_rows] for x in new_rows], axis=0
            )
            fresh[b * LANES : (b + 1) * LANES, :] = jnp.dot(
                spread_out, stack, preferred_element_type=f32
            ).astype(narrow)
        out_width = wo.shape[1]
        wo_load.wait()
        routes()
        out_core, out_home = {}, {}

        def forward_heads(d):
            for h in range(kv_heads):
                head_group[h, d].wait_recv()
                landed = heads.at[group_from(d), rank, :, head_columns[h]]
                for r in near_ranks:
                    head_rank[h, d, r] = go(landed, landed, rank_place(r))

        def project_out(d):
            source = group_from(d)
            for h in range(kv_heads):
                for r in near_ranks:
                    head_rank[h, d, r].wait_recv()
            part_out[source] = (
                jnp.dot(
                    heads[source].reshape(ranks * span, heads.shape[3]),
                    wo[...],
                    preferred_element_type=f32,
                )
                .astype(narrow)
                .reshape(ranks, cores, half, out_width)
            )
            out_core[d] = go(part_out.at[source, :, 1 - mdl], near_out.at[source], other)

        def send_out(d):
            source = group_from(d)
            out_core[d].wait_recv()
            for r in every_rank:
                giver = rank_from(r)
                total = part_out[source, giver, mdl].astype(f32) + near_out[source, giver].astype(f32)
                if d or r:
                    part_out[source, giver, mdl] = total.astype(narrow)
                    out_home[d, r] = go(
                        part_out.at[source, giver, mdl],
                        in_out.at[tok],
                        place(source * ranks + giver, mdl),
                    )
                else:
                    in_out[tok] = total.astype(narrow)

        for s in range(groups + 2):
            if 0 < s < groups:
                forward_heads(order[s])
            if 0 <= s - 1 < groups:
                project_out(order[s - 1])
            if 0 <= s - 2 < groups:
                send_out(order[s - 2])
        for d in order:
            for r in every_rank:
                if d or r:
                    out_home[d, r].wait_recv()
        square = jnp.zeros((half, 1), f32)
        for t in range(toks):
            at = pl.ds(t * depth, depth)
            total = full[:, at].astype(f32) + in_out[t].astype(f32)
            resid[:, at] = total
            square += jnp.sum(total * total, axis=1, keepdims=True)
        row_scale = lax.rsqrt(square * (1.0 / width) + eps_norm)
        all_sent()
        for b in range(width // LANES):
            at = pl.ds(b * LANES, LANES)
            gain = gains[width // LANES + b : width // LANES + b + 1, :]
            full[:, at] = (resid[:, at] * row_scale * gain).astype(narrow)

    def mix(rows, gate_acc, up_acc, slab):
        tokens = full
        rest = cap - main
        packed = cut(send.shape[2], pieces)
        blocks = part // LANES
        main_rows = cores * toks * main
        tile = divide(hidden_units)

        def pack(target, lead, rows_in, row, c):
            for b in range(blocks):
                spot, lane = divmod(b, main // rest)
                at = c * (send.shape[2] // pieces) + part + spot * LANES
                target[(*lead, pl.ds(lane * rest, rest), pl.ds(at, LANES))] = rows_in[
                    row : row + rest, b * LANES : (b + 1) * LANES
                ]

        def unpack(target, row, source, lead, c):
            for b in range(blocks):
                spot, lane = divmod(b, main // rest)
                at = c * (send.shape[2] // pieces) + part + spot * LANES
                target[row : row + rest, b * LANES : (b + 1) * LANES] = source[
                    (*lead, pl.ds(lane * rest, rest), pl.ds(at, LANES))
                ]

        def body(c):
            return pl.ds(c * (send.shape[2] // pieces), part)

        by_group, by_rank, by_core = {}, {}, {}
        for c in range(pieces):
            picked = jnp.dot(
                picks[...], tokens[:, columns[c]], preferred_element_type=jnp.float32
            ).astype(send.dtype)
            for e in range(groups):
                send[e, :, body(c)] = picked[e * main : (e + 1) * main]
                pack(send, (e,), picked, groups * main + e * rest, c)
            for d in far:
                by_group[c, d] = go(
                    send.at[(group + d) % groups, :, packed[c]],
                    recv.at[mdl, group, rank, :, packed[c]],
                    group_place(d),
                )
            for r in near_ranks:
                by_rank[c, 0, r] = go(
                    send.at[group, :, packed[c]],
                    recv.at[mdl, group, rank, :, packed[c]],
                    rank_place(r),
                )
            by_core[c, 0, 0] = go(
                send.at[group, :, packed[c]], recv.at[mdl, group, rank, :, packed[c]], other
            )

        recv[mdl, group, rank] = send[group]

        def from_groups(c):
            for d in far:
                by_group[c, d].wait_recv()
                source = (group + groups - d) % groups
                block = recv.at[mdl, source, rank, :, packed[c]]
                for r in near_ranks:
                    by_rank[c, d, r] = go(block, block, rank_place(r))
                by_core[c, d, 0] = go(block, block, other)

        def from_ranks(c):
            for d in [0] + far:
                for r in near_ranks:
                    by_rank[c, d, r].wait_recv()
                    source = (group + groups - d) % groups
                    giver = (rank + ranks - r) % ranks
                    block = recv.at[mdl, source, giver, :, packed[c]]
                    by_core[c, d, r] = go(block, block, other)

        def assemble(c):
            for d in [0] + far:
                for r in [0] + near_ranks:
                    by_core[c, d, r].wait_recv()
            rows[0:main_rows, :] = recv[:, :, :, :, body(c)].reshape(main_rows, part)
            spot = main_rows
            for m in range(cores):
                for g in range(groups):
                    for r in range(ranks):
                        unpack(rows, spot, recv, (m, g, r), c)
                        spot += rest

        def project(c):
            assemble(c)
            load_gate(c).wait()
            load_up(c).wait()

            def step(n, carry):
                at = pl.ds(pl.multiple_of(n * tile, tile), tile)
                x = rows[...]
                gate_val = jnp.dot(x, gate_w[columns[c], at], preferred_element_type=jnp.float32)
                up_val = jnp.dot(x, up_w[columns[c], at], preferred_element_type=jnp.float32)
                if c > 0:
                    gate_val = gate_val + gate_acc[:, at]
                    up_val = up_val + up_acc[:, at]
                if c < pieces - 1:
                    gate_acc[:, at] = gate_val
                    up_acc[:, at] = up_val
                else:
                    slab[:, at] = (gate_val / (1.0 + jnp.exp(-gate_val)) * up_val).astype(slab.dtype)
                return carry

            lax.fori_loop(0, hidden_units // tile, step, 0)

        for s in range(pieces + 2):
            if s < pieces:
                from_groups(s)
            if 0 <= s - 1 < pieces:
                from_ranks(s - 1)
            if 0 <= s - 2 < pieces:
                project(s - 2)

        all_sent()
        down_tile = divide(part)
        across, to_rank, to_home = {}, {}, {}

        def down(c):
            load_down(c).wait()

            def step(n, carry):
                at = pl.multiple_of(n * down_tile, down_tile)
                rows[:, pl.ds(at, down_tile)] = jnp.dot(
                    slab[...],
                    down_w[c, :, pl.ds(at, down_tile)],
                    preferred_element_type=jnp.float32,
                ).astype(rows.dtype)
                return carry

            lax.fori_loop(0, part // down_tile, step, 0)
            recv[:, :, :, :, body(c)] = rows[0:main_rows, :].reshape(cores, groups, ranks, main, part)
            spot = main_rows
            for m in range(cores):
                for g in range(groups):
                    for r in range(ranks):
                        pack(recv, (m, g, r), rows, spot, c)
                        spot += rest
            across[c] = go(
                recv.at[1 - mdl, :, :, :, packed[c]], near.at[:, :, :, packed[c]], other
            )

        def pair(g, r, c):
            return recv[mdl, g, r, :, packed[c]].astype(jnp.float32) + near[
                g, r, :, packed[c]
            ].astype(jnp.float32)

        def to_ranks(c):
            across[c].wait_recv()
            for r in near_ranks:
                there = (rank + r) % ranks
                for g in range(groups):
                    recv[mdl, g, there, :, packed[c]] = pair(g, there, c).astype(recv.dtype)
                to_rank[c, r] = go(
                    recv.at[mdl, :, there, :, packed[c]], mid.at[r - 1, :, :, packed[c]], rank_place(r)
                )

        def to_sources(c):
            for r in near_ranks:
                to_rank[c, r].wait_recv()
            for d in far[::-1] + [0]:
                there = (group + d) % groups
                total = pair(there, rank, c)
                for r in near_ranks:
                    total = total + mid[r - 1, there, :, packed[c]].astype(jnp.float32)
                if d == 0:
                    home[group, :, packed[c]] = total.astype(home.dtype)
                else:
                    recv[mdl, there, rank, :, packed[c]] = total.astype(recv.dtype)
                    to_home[c, d] = go(
                        recv.at[mdl, there, rank, :, packed[c]],
                        home.at[group, :, packed[c]],
                        group_place(d),
                    )

        def finish(c):
            for d in far:
                to_home[c, d].wait_recv()
            rows[0 : groups * main, :] = home[:, :, body(c)].reshape(groups * main, part)
            for e in range(groups):
                unpack(rows, groups * main + e * rest, home, (e,), c)
            terms = jnp.dot(
                weights[...], rows[0 : groups * cap, :], preferred_element_type=jnp.float32
            )
            total = resid[:, columns[c]]
            for k in range(weights.shape[0] // resid.shape[0]):
                total = total + terms[k * resid.shape[0] : (k + 1) * resid.shape[0]]
            mixed[:, columns[c]] = total.astype(mixed.dtype)

        lag_rank, lag_source, lag_end = 1, 2, 4
        for s in range(pieces + lag_end):
            if s < pieces:
                down(s)
            if 0 <= s - lag_rank < pieces:
                to_ranks(s - lag_rank)
            if 0 <= s - lag_source < pieces:
                to_sources(s - lag_source)
            if 0 <= s - lag_end < pieces:
                finish(s - lag_end)

    scoped = [
        (cache_hbm.shape, narrow),
        (wkv_hbm.shape, narrow),
        ((query_heads, span, head_dim), narrow),
        ((kv_heads, 2, limit, head_dim), narrow),
        ((depth, 2 * kv_heads * head_dim), narrow),
        (wo_hbm.shape, narrow),
        ((kv_heads, query_count, head_dim), f32),
        ((kv_heads, query_count, head_dim), f32),
        ((kv_heads, query_count, head_dim), f32),
    ]
    pl.run_scoped(first_part, *[pltpu.VMEM(shape, kind) for shape, kind in scoped])
    scoped = [
        ((total_rows, part), narrow),
        ((total_rows, hidden_units), f32),
        ((total_rows, hidden_units), f32),
        ((total_rows, hidden_units), narrow),
    ]
    pl.run_scoped(second_part, *[pltpu.VMEM(shape, kind) for shape, kind in scoped])


def layer(
    dims,
    lengths,
    hidden,
    queries,
    cosines,
    sines,
    gains,
    cache,
    wkv,
    wo,
    w_gate,
    w_up,
    w_down,
):
    groups, ranks, cores, pieces, kv_heads = dims
    toks = groups * ranks
    span, features = hidden.shape
    half, width = span // cores, features * cores
    cap = half * TOPK * 9 // (8 * groups)
    main = cap // 16 * 16
    packed = width // main * cap
    depth, units = w_gate.shape[1:]
    part = width // pieces
    head_dim = queries.shape[1]
    kv_width, out_width = 2 * kv_heads * head_dim, wo.shape[1]
    depth_slice = width // toks
    dtype, f32 = hidden.dtype, jnp.float32
    more = max(ranks - 1, 1)
    copies = (
        2
        + (2 * toks - 1)
        + groups * (ranks - 1)
        + groups
        - 1
        + kv_heads * (groups - 1 + groups * (ranks - 1))
        + groups
        + toks
        - 1
        + pieces * ((groups - 1) * 2 + (groups + 1) * (ranks - 1) + toks + 1)
    )
    remote_space = pl.BlockSpec(memory_space=pl.ANY)
    buffers = [
        ((half, width), dtype),
        ((groups, ranks, cores, half, depth_slice), dtype),
        ((span, head_dim), f32),
        ((span, head_dim), f32),
        ((groups, ranks, span, kv_width), dtype),
        ((more, groups, span, kv_width), dtype),
        ((groups, span, kv_width), dtype),
        ((groups, span, kv_width), dtype),
        ((groups, ranks, span, wo.shape[0]), dtype),
        ((groups, ranks, cores, half, out_width), dtype),
        ((groups, ranks, half, out_width), dtype),
        ((toks, half, out_width), dtype),
        ((half, width), f32),
        ((groups, main, packed), dtype),
        ((cores, groups, ranks, main, packed), dtype),
        ((groups, ranks, main, packed), dtype),
        ((more, groups, main, packed), dtype),
        ((groups, main, packed), dtype),
        ((depth, units), dtype),
        ((depth, units), dtype),
        ((pieces, units, part), dtype),
        ((groups * cap, half), dtype),
        ((3 * half, groups * cap), dtype),
    ]
    return pl.pallas_call(
        functools.partial(layer_kernel, dims),
        out_shape=(
            jax.ShapeDtypeStruct((half, width), dtype),
            jax.ShapeDtypeStruct((span * 2 * kv_heads, head_dim), dtype),
        ),
        in_specs=[pl.BlockSpec(memory_space=pltpu.SMEM)] + [VMEM] * 5 + [remote_space] * 6,
        out_specs=(VMEM, VMEM),
        scratch_shapes=[pltpu.VMEM(shape, kind) for shape, kind in buffers]
        + [
            pltpu.SemaphoreType.DMA((2, copies)),
            pltpu.SemaphoreType.DMA((3 * pieces + 4,)),
        ],
        compiler_params=pltpu.CompilerParams(
            collective_id=1, has_side_effects=True, vmem_limit_bytes=67043328
        ),
    )(
        lengths,
        hidden,
        queries,
        cosines,
        sines,
        gains,
        cache,
        wkv,
        wo,
        w_gate,
        w_up,
        w_down,
    )


def shards(
    hidden,
    queries,
    cache,
    cache_lengths,
    wkv,
    wo,
    attn_gain,
    moe_gain,
    w_gate,
    w_up,
    w_down,
    expert_ids,
    gates,
):
    span_len = hidden.shape[0]
    toks = lax.axis_size("tok")
    core_count = lax.axis_size("mdl")
    ranks = toks // EXPERTS
    kv_heads, _, head_dim = wkv.shape[1:]
    positions = cache_lengths[0] + jnp.arange(span_len, dtype=jnp.int32)
    cosines, sines = rotation(head_dim, positions)
    named = jnp.concatenate([expert_ids.astype(jnp.float32), gates], axis=1)
    gains = jnp.concatenate(
        [
            jnp.concatenate([attn_gain, moe_gain]).astype(jnp.float32).reshape(-1, LANES),
            jnp.pad(named, ((0, 0), (0, LANES - named.shape[1]))),
        ]
    )
    mixed, fresh = layer(
        (EXPERTS, ranks, core_count, PIECES, kv_heads),
        cache_lengths,
        hidden,
        queries.reshape(-1, head_dim),
        cosines,
        sines,
        gains,
        cache.reshape(-1, head_dim),
        wkv.reshape(-1, head_dim),
        wo.reshape(-1, wo.shape[2]),
        w_gate,
        w_up,
        w_down,
    )
    fresh_key_value = fresh.reshape(span_len, kv_heads, 2, head_dim)
    return (mixed, fresh_key_value)


def solution(mesh):
    in_specs = (
        P(("grp", "tok"), "mdl"),
        P(("grp", "tok"), "mdl", None),
        P(("grp", "tok"), None, "mdl", None, None),
        P(("grp", "tok")),
        P("tok", "mdl", None, None),
        P("mdl", None, "tok"),
        P(),
        P(),
        P(("tok", "mdl"), None, None),
        P(("tok", "mdl"), None, None),
        P(("tok", "mdl"), None, None),
        P(("grp", "tok", "mdl"), None),
        P(("grp", "tok", "mdl"), None),
    )
    out_specs = (P(("grp", "tok", "mdl"), None), P(("grp", "tok"), "mdl", None, None))
    return jax.shard_map(shards, mesh=mesh, in_specs=in_specs, out_specs=out_specs, check_vma=False)
```
